8 devices in a mesh: dp: 1 (over z), ep: 8 (over y, x, core).
Axes of the slice: x: 2, y: 2, z: 1, core: 2. Of those that a mesh axis runs over, the one named last changes fastest.
Arguments:
- tokens: bfloat16 [8, 1024, 1024], P(('dp', 'ep'))
- w_gate: bfloat16 [1024, 32], replicated
- expert_ids: int32 [8, 1024, 2], P(('dp', 'ep'))
- keep_second: int32 [8, 1024], P(('dp', 'ep'))
- w_in: bfloat16 [32, 1024, 2816], P('ep')
- w_out: bfloat16 [32, 2816, 1024], P('ep')
Outputs:
- output: bfloat16 [8, 1024, 1024], P(('dp', 'ep'))
All inputs are finite; a program needn't handle non-finite values.
Results may differ from the reference program's by a relative error of at most 0.001.
Values are sent between devices in bfloat16 or wider.
A program may use at most 1 GiB of HBM per device.

```python
import functools
import jax
import jax.numpy as jnp
from jax import lax

GROUPS = 8
TOKENS = 1024
MODEL_DIM = 1024
HIDDEN = 2816
EXPERTS = 32
CAPACITY = 2 * TOKENS // EXPERTS


def draw_routing(route_key):
    k_cover, k_raw, k_shift, k_second, k_keep = jax.random.split(route_key, 5)
    cover_keys = jax.random.split(k_cover, GROUPS)
    cover_ids = jax.vmap(functools.partial(jax.random.permutation, x=EXPERTS))(cover_keys)
    hot_shift = jax.random.randint(k_shift, (), 0, EXPERTS)
    raw_ids = jax.random.randint(k_raw, (GROUPS, TOKENS - EXPERTS), 0, EXPERTS + EXPERTS // 2)
    rest_ids = (raw_ids % EXPERTS + hot_shift) % EXPERTS
    first_ids = jnp.concatenate([cover_ids.astype(jnp.int32), rest_ids.astype(jnp.int32)], axis=1)
    second_ids = (first_ids + jax.random.randint(k_second, (GROUPS, TOKENS), 1, EXPERTS)) % EXPERTS
    keep_second = (jax.random.randint(k_keep, (GROUPS, TOKENS), 0, 10) < 9).astype(jnp.int32)
    expert_ids = jnp.stack([first_ids, second_ids], axis=-1).astype(jnp.int32)
    return expert_ids, keep_second


def setup_inputs(seed: int = 0, part: int = 0) -> dict:
    shared_key, parts_key = jax.random.split(jax.random.key(seed))
    part_key = jax.random.fold_in(parts_key, part)
    k_tokens, k_route = jax.random.split(part_key)
    k_gate, k_in, k_out = jax.random.split(shared_key, 3)
    tokens = jax.random.normal(k_tokens, (GROUPS, TOKENS, MODEL_DIM), jnp.float32).astype(jnp.bfloat16)
    expert_ids, keep_second = draw_routing(k_route)
    w_gate = (jax.random.normal(k_gate, (MODEL_DIM, EXPERTS), jnp.float32) * MODEL_DIM ** -0.5).astype(jnp.bfloat16)
    w_in = (jax.random.normal(k_in, (EXPERTS, MODEL_DIM, HIDDEN), jnp.float32) * MODEL_DIM ** -0.5).astype(jnp.bfloat16)
    w_out = (jax.random.normal(k_out, (EXPERTS, HIDDEN, MODEL_DIM), jnp.float32) * (2.0 / HIDDEN) ** 0.5).astype(jnp.bfloat16)
    return {"tokens": tokens, "w_gate": w_gate, "expert_ids": expert_ids, "keep_second": keep_second, "w_in": w_in, "w_out": w_out}


def group_routing(group_tok, group_ids, group_keep, w_gate):
    logits = jnp.dot(group_tok, w_gate, preferred_element_type=jnp.float32)
    gate_probs = jax.nn.softmax(logits, axis=-1)
    first_hot = jax.nn.one_hot(group_ids[:, 0], EXPERTS, dtype=jnp.int32)
    second_hot = jax.nn.one_hot(group_ids[:, 1], EXPERTS, dtype=jnp.int32) * group_keep[:, None]
    gate_first = jnp.sum(gate_probs * first_hot, axis=-1)
    gate_second = jnp.sum(gate_probs * second_hot, axis=-1)
    gate_total = gate_first + gate_second
    gate_first = gate_first / gate_total
    gate_second = gate_second / gate_total
    pos_first = jnp.sum((jnp.cumsum(first_hot, axis=0) - first_hot) * first_hot, axis=-1)
    second_base = jnp.cumsum(second_hot, axis=0) - second_hot + jnp.sum(first_hot, axis=0)[None, :]
    pos_second = jnp.sum(second_base * second_hot, axis=-1)
    slot_first = first_hot[:, :, None] * jax.nn.one_hot(pos_first, CAPACITY, dtype=jnp.float32)[:, None, :]
    slot_second = second_hot[:, :, None] * jax.nn.one_hot(pos_second, CAPACITY, dtype=jnp.float32)[:, None, :]
    dispatch = slot_first + slot_second
    combine = (gate_first[:, None, None] * slot_first + gate_second[:, None, None] * slot_second).astype(jnp.bfloat16)
    return dispatch, combine


def reference(tokens, w_gate, expert_ids, keep_second, w_in, w_out):
    def dispatch_group(operands):
        group_tok, group_ids, group_keep = operands
        dispatch, _ = group_routing(group_tok, group_ids, group_keep, w_gate)
        sent_rows = jnp.einsum("sec,sm->ecm", dispatch.astype(jnp.float32), group_tok.astype(jnp.float32))
        return sent_rows.astype(jnp.bfloat16)

    expert_in = lax.map(dispatch_group, (tokens, expert_ids, keep_second))
    expert_in = jnp.transpose(expert_in, (1, 0, 2, 3))

    def expert_ffn(operands):
        rows_in, w_first, w_second = operands
        flat_rows = rows_in.reshape(GROUPS * CAPACITY, MODEL_DIM)
        hidden = jax.nn.relu(jnp.dot(flat_rows, w_first, preferred_element_type=jnp.float32)).astype(jnp.bfloat16)
        rows_out = jnp.dot(hidden, w_second, preferred_element_type=jnp.float32).astype(jnp.bfloat16)
        return rows_out.reshape(GROUPS, CAPACITY, MODEL_DIM)

    expert_out = lax.map(expert_ffn, (expert_in, w_in, w_out))
    expert_out = jnp.transpose(expert_out, (1, 0, 2, 3))

    def combine_group(operands):
        group_tok, group_ids, group_keep, rows_back = operands
        _, combine = group_routing(group_tok, group_ids, group_keep, w_gate)
        mixed_rows = jnp.einsum("sec,ecm->sm", combine.astype(jnp.float32), rows_back.astype(jnp.float32))
        return mixed_rows.astype(jnp.bfloat16)

    return lax.map(combine_group, (tokens, expert_ids, keep_second, expert_out))
```

```python
import functools

import jax
import jax.numpy as jnp
from jax import lax
from jax.experimental import pallas as pl
from jax.experimental.pallas import tpu as pltpu
from jax.sharding import PartitionSpec as P

MESH = pl.DeviceIdType.MESH
SEND_ORDER = (6, 7, 2, 4, 3, 5, 1)


def peer_of(me, k):
    core, x, y = me % 2, (me // 2) % 2, me // 4
    core_bit, x_bit, y_bit = k % 2, (k // 2) % 2, k // 4
    core = 1 - core if core_bit else core
    x = 1 - x if x_bit else x
    y = 1 - y if y_bit else y
    return (y * 2 + x) * 2 + core


def layer_kernel(
    cap, tok_hbm, wg_hbm, ids_hbm, keep_hbm, win_hbm, wout_hbm, out_hbm,
    tok, wg, ids, keep, keys, gates, cols, dmat, xs, xr, ys, yr, hid, wi, wo, cw, acc, obuf,
    in_sem, wi_sem, wo_sem, xs_sem, xr_sem, ys_sem, yr_sem, out_sem,
):
    me = lax.axis_index("ep")
    experts_here = win_hbm.shape[0]
    tokens, dim = tok.shape
    experts = wg.shape[0]
    hidden = hid.shape[1]
    groups = experts // experts_here
    rows = groups * cap
    f32, bf16 = jnp.float32, jnp.bfloat16

    barrier = pltpu.get_barrier_semaphore()
    for k in range(1, 8):
        pl.semaphore_signal(barrier, inc=1, device_id={"ep": peer_of(me, k)}, device_id_type=MESH)

    small = [
        pltpu.make_async_copy(ids_hbm, ids, in_sem.at[0]),
        pltpu.make_async_copy(keep_hbm, keep, in_sem.at[1]),
        pltpu.make_async_copy(tok_hbm, tok, in_sem.at[2]),
        pltpu.make_async_copy(wg_hbm, wg, in_sem.at[3]),
    ]
    for copy in small:
        copy.start()

    def wi_copy(e):
        return pltpu.make_async_copy(win_hbm.at[e], wi.at[e % 2], wi_sem.at[e % 2])

    def wo_copy(e):
        return pltpu.make_async_copy(wout_hbm.at[e], wo.at[e % 2], wo_sem.at[e % 2])

    for e in range(2):
        wi_copy(e).start()
        wo_copy(e).start()

    small[0].wait()
    small[1].wait()
    expert_row = lax.broadcasted_iota(jnp.int32, (experts, tokens), 0)
    id1, id2, kept2 = ids[0:1, :], ids[1:2, :], keep[0:1, :]
    hot1 = (expert_row == id1).astype(f32)
    hot2 = ((expert_row == id2) & (kept2 > 0)).astype(f32)
    hot = jnp.concatenate([hot1, hot2], axis=0).astype(bf16)
    blk = 256
    r_io = lax.broadcasted_iota(jnp.int32, (blk, blk), 0)
    c_io = lax.broadcasted_iota(jnp.int32, (blk, blk), 1)
    before = jnp.where(r_io < c_io, 1.0, 0.0).astype(bf16)
    ones = jnp.ones((blk, blk), bf16)
    seen = jnp.zeros((2 * experts, blk), f32)
    earlier = []
    for b in range(tokens // blk):
        part = hot[:, b * blk:(b + 1) * blk]
        earlier.append(jnp.dot(part, before, preferred_element_type=f32) + seen)
        seen = seen + jnp.dot(part, ones, preferred_element_type=f32)
    first_total = seen[:experts, :]
    pos1 = jnp.concatenate([jnp.sum(p[:experts] * hot1[:, b * blk:(b + 1) * blk], axis=0, keepdims=True) for b, p in enumerate(earlier)], axis=1)
    pos2 = jnp.concatenate([jnp.sum((p[experts:] + first_total) * hot2[:, b * blk:(b + 1) * blk], axis=0, keepdims=True) for b, p in enumerate(earlier)], axis=1)
    pos1, pos2 = pos1.astype(jnp.int32), pos2.astype(jnp.int32)
    key1 = jnp.where(pos1 < cap, id1 * cap + pos1, -1)
    key2 = jnp.where((pos2 < cap) & (kept2 > 0), id2 * cap + pos2, -1)
    keys[0:1, :] = key1
    keys[1:2, :] = key2

    def x_send(e, k):
        peer = peer_of(me, k)
        return pltpu.make_async_remote_copy(
            src_ref=xs.at[e, pl.ds(pl.multiple_of(peer * cap, cap), cap)],
            dst_ref=xr.at[e, pl.ds(pl.multiple_of(me * cap, cap), cap)],
            send_sem=xs_sem.at[e, k], recv_sem=xr_sem.at[e, k],
            device_id={"ep": peer}, device_id_type=MESH,
        )

    def y_send(e, k):
        peer = peer_of(me, k)
        return pltpu.make_async_remote_copy(
            src_ref=ys.at[e, pl.ds(pl.multiple_of(peer * cap, cap), cap)],
            dst_ref=yr.at[e, pl.ds(pl.multiple_of(me * cap, cap), cap)],
            send_sem=ys_sem.at[e, k], recv_sem=yr_sem.at[e, k],
            device_id={"ep": peer}, device_id_type=MESH,
        )

    mine = pl.ds(pl.multiple_of(me * cap, cap), cap)

    def dispatch(e):
        row = lax.broadcasted_iota(jnp.int32, (rows, tokens), 0)
        slot = (row // cap) * (experts_here * cap) + e * cap + row % cap
        hit = (slot == keys[0:1, :]) | (slot == keys[1:2, :])
        dmat[...] = jnp.where(hit, 1.0, 0.0).astype(bf16)

        def columns(n, _):
            at = pl.ds(pl.multiple_of(n * blk, blk), blk)
            xs[e, :, at] = jnp.dot(dmat[...], tok[:, at], preferred_element_type=f32).astype(bf16)
            return 0

        lax.fori_loop(0, dim // blk, columns, 0)
        xr[e, mine] = xs[e, mine]

    small[2].wait()
    dispatch(0)
    pl.semaphore_wait(barrier, 7)
    for k in SEND_ORDER:
        x_send(0, k).start()

    def dispatch_rest(e, _):
        dispatch(e)
        for k in SEND_ORDER:
            x_send(e, k).start()
        return 0

    lax.fori_loop(1, experts_here, dispatch_rest, 0)

    small[3].wait()
    logits = lax.dot_general(wg[...], tok[...], (((1,), (1,)), ((), ())), preferred_element_type=f32)
    top = jnp.max(logits, axis=0, keepdims=True)
    expd = jnp.exp(logits - top)
    probs = expd / jnp.sum(expd, axis=0, keepdims=True)
    gate1 = jnp.sum(jnp.where(expert_row == ids[0:1, :], probs, 0.0), axis=0, keepdims=True)
    gate2 = jnp.sum(jnp.where((expert_row == ids[1:2, :]) & (keep[0:1, :] > 0), probs, 0.0), axis=0, keepdims=True)
    total = gate1 + gate2
    gates[0:1, :] = keys[0:1, :].astype(f32)
    gates[1:2, :] = keys[1:2, :].astype(f32)
    gates[2:3, :] = gate1 / total
    gates[3:4, :] = gate2 / total
    gates[4:, :] = jnp.zeros((gates.shape[0] - 4, tokens), f32)
    cols[...] = gates[...].T

    def weights(e, _):
        def block(t, _):
            at = pl.ds(pl.multiple_of(t * blk, blk), blk)
            lane = lax.broadcasted_iota(jnp.int32, (blk, rows), 1)
            slot = ((lane // cap) * (experts_here * cap) + e * cap + lane % cap).astype(f32)
            part = cols[at, :]
            cw[e, at, :] = (
                jnp.where(slot == part[:, 0:1], part[:, 2:3], 0.0) + jnp.where(slot == part[:, 1:2], part[:, 3:4], 0.0)
            ).astype(bf16)
            return 0

        return lax.fori_loop(0, tokens // blk, block, 0)

    lax.fori_loop(0, experts_here, weights, 0)

    def expert(e, _):
        s = e % 2
        for k in SEND_ORDER:
            x_send(e, k).wait_recv()
        wi_copy(e).wait()

        def up(j, _):
            at = pl.ds(pl.multiple_of(j * blk, blk), blk)
            pre = jnp.dot(xr[e], wi[s, :, at], preferred_element_type=f32)
            hid[:, at] = jnp.maximum(pre, 0.0).astype(bf16)
            return 0

        lax.fori_loop(0, hidden // blk, up, 0)

        @pl.when(e + 2 < experts_here)
        def _():
            wi_copy(e + 2).start()

        wo_copy(e).wait()

        def down(n, _):
            at = pl.ds(pl.multiple_of(n * blk, blk), blk)
            ys[e, :, at] = jnp.dot(hid[...], wo[s, :, at], preferred_element_type=f32).astype(bf16)
            return 0

        lax.fori_loop(0, dim // blk, down, 0)

        @pl.when(e + 2 < experts_here)
        def _():
            wo_copy(e + 2).start()

        for k in SEND_ORDER:
            y_send(e, k).start()
        yr[e, mine] = ys[e, mine]
        return 0

    lax.fori_loop(0, experts_here, expert, 0)

    def back(e):
        for k in SEND_ORDER:
            y_send(e, k).wait_recv()

    back(0)

    def first_columns(n, _):
        at = pl.ds(pl.multiple_of(n * blk, blk), blk)
        acc[:, at] = jnp.dot(cw[0], yr[0, :, at], preferred_element_type=f32)
        return 0

    lax.fori_loop(0, dim // blk, first_columns, 0)

    def combine(e, _):
        back(e)

        def columns(n, _):
            at = pl.ds(pl.multiple_of(n * blk, blk), blk)
            acc[:, at] += jnp.dot(cw[e], yr[e, :, at], preferred_element_type=f32)
            return 0

        return lax.fori_loop(0, dim // blk, columns, 0)

    lax.fori_loop(1, experts_here - 1, combine, 0)
    last = experts_here - 1
    back(last)

    def out_copy(t):
        at = pl.ds(pl.multiple_of(t * blk, blk), blk)
        return pltpu.make_async_copy(obuf.at[at], out_hbm.at[at], out_sem.at[t])

    def finish(t, _):
        at = pl.ds(pl.multiple_of(t * blk, blk), blk)
        obuf[at, :] = (acc[at, :] + jnp.dot(cw[last, at, :], yr[last], preferred_element_type=f32)).astype(bf16)
        out_copy(t).start()
        return 0

    lax.fori_loop(0, tokens // blk, finish, 0)

    def drain(e, _):
        for k in SEND_ORDER:
            x_send(e, k).wait_send()
            y_send(e, k).wait_send()
        return 0

    lax.fori_loop(0, experts_here, drain, 0)
    for t in range(tokens // blk):
        out_copy(t).wait()


def solution(mesh):
    def local_layer(tokens, w_gate, expert_ids, keep_second, w_in, w_out):
        _, token_count, dim = tokens.shape
        experts = w_gate.shape[1]
        here, _, hidden = w_in.shape
        cap = 2 * token_count // experts
        groups = experts // here
        rows = groups * cap
        f32, bf16 = jnp.float32, jnp.bfloat16
        vmem, dma = pltpu.VMEM, pltpu.SemaphoreType.DMA
        out = pl.pallas_call(
            functools.partial(layer_kernel, cap),
            out_shape=jax.ShapeDtypeStruct((token_count, dim), bf16),
            in_specs=[pl.BlockSpec(memory_space=pl.ANY)] * 6,
            out_specs=pl.BlockSpec(memory_space=pl.ANY),
            scratch_shapes=[
                vmem((token_count, dim), bf16),
                vmem((experts, dim), bf16),
                vmem((2, token_count), jnp.int32),
                vmem((1, token_count), jnp.int32),
                vmem((8, token_count), jnp.int32),
                vmem((128, token_count), f32),
                vmem((token_count, 128), f32),
                vmem((rows, token_count), bf16),
                vmem((here, rows, dim), bf16),
                vmem((here, rows, dim), bf16),
                vmem((here, rows, dim), bf16),
                vmem((here, rows, dim), bf16),
                vmem((rows, hidden), bf16),
                vmem((2, dim, hidden), bf16),
                vmem((2, hidden, dim), bf16),
                vmem((here, token_count, rows), bf16),
                vmem((token_count, dim), f32),
                vmem((token_count, dim), bf16),
                dma((4,)), dma((2,)), dma((2,)),
                dma((here, groups)), dma((here, groups)), dma((here, groups)), dma((here, groups)),
                dma((4,)),
            ],
            compiler_params=pltpu.CompilerParams(collective_id=0, has_side_effects=True, vmem_limit_bytes=67043328),
            name="moe_layer",
        )(tokens[0], w_gate.T, expert_ids[0].T, keep_second, w_in, w_out)
        return out[None]

    group_spec = P(("dp", "ep"))
    return jax.shard_map(local_layer, mesh=mesh, in_specs=(group_spec, P(), group_spec, group_spec, P("ep"), P("ep")), out_specs=group_spec, check_vma=False)
```

```python
import functools

import jax
import jax.numpy as jnp
from jax import lax
from jax.experimental import pallas as pl
from jax.experimental.pallas import tpu as pltpu
from jax.sharding import PartitionSpec as P

MESH = pl.DeviceIdType.MESH
SEND_ORDER = (6, 7, 2, 4, 3, 5, 1)


def peer_of(me, k):
    core, x, y = me % 2, (me // 2) % 2, me // 4
    core_bit, x_bit, y_bit = k % 2, (k // 2) % 2, k // 4
    core = 1 - core if core_bit else core
    x = 1 - x if x_bit else x
    y = 1 - y if y_bit else y
    return (y * 2 + x) * 2 + core


def layer_kernel(
    cap, tok_hbm, wg_hbm, ids_hbm, keep_hbm, win_hbm, wout_hbm, obuf,
    tok, wg, ids, keep, keys, gates, cols, dmat, xs, xr, ys, yr, hid, wi, wo, cw, acc,
    in_sem, wi_sem, wo_sem, xs_sem, xr_sem, ys_sem, yr_sem,
):
    me = lax.axis_index("ep")
    experts_here = win_hbm.shape[0]
    tokens, dim = tok.shape
    experts = wg.shape[0]
    hidden = hid.shape[1]
    groups = experts // experts_here
    rows = groups * cap
    f32, bf16 = jnp.float32, jnp.bfloat16

    barrier = pltpu.get_barrier_semaphore()
    for k in range(1, 8):
        pl.semaphore_signal(barrier, inc=1, device_id={"ep": peer_of(me, k)}, device_id_type=MESH)

    small = [
        pltpu.make_async_copy(ids_hbm, ids, in_sem.at[0]),
        pltpu.make_async_copy(keep_hbm, keep, in_sem.at[1]),
        pltpu.make_async_copy(tok_hbm, tok, in_sem.at[2]),
        pltpu.make_async_copy(wg_hbm, wg, in_sem.at[3]),
    ]
    for copy in small:
        copy.start()

    def wi_copy(e):
        return pltpu.make_async_copy(win_hbm.at[e], wi.at[e % 2], wi_sem.at[e % 2])

    def wo_copy(e):
        return pltpu.make_async_copy(wout_hbm.at[e], wo.at[e % 2], wo_sem.at[e % 2])

    for e in range(2):
        wi_copy(e).start()
        wo_copy(e).start()

    small[0].wait()
    small[1].wait()
    expert_row = lax.broadcasted_iota(jnp.int32, (experts, tokens), 0)
    id1, id2, kept2 = ids[0:1, :], ids[1:2, :], keep[0:1, :]
    hot1 = (expert_row == id1).astype(f32)
    hot2 = ((expert_row == id2) & (kept2 > 0)).astype(f32)
    hot = jnp.concatenate([hot1, hot2], axis=0).astype(bf16)
    blk = 256
    r_io = lax.broadcasted_iota(jnp.int32, (blk, blk), 0)
    c_io = lax.broadcasted_iota(jnp.int32, (blk, blk), 1)
    before = jnp.where(r_io < c_io, 1.0, 0.0).astype(bf16)
    ones = jnp.ones((blk, blk), bf16)
    seen = jnp.zeros((2 * experts, blk), f32)
    earlier = []
    for b in range(tokens // blk):
        part = hot[:, b * blk:(b + 1) * blk]
        earlier.append(jnp.dot(part, before, preferred_element_type=f32) + seen)
        seen = seen + jnp.dot(part, ones, preferred_element_type=f32)
    first_total = seen[:experts, :]
    pos1 = jnp.concatenate([jnp.sum(p[:experts] * hot1[:, b * blk:(b + 1) * blk], axis=0, keepdims=True) for b, p in enumerate(earlier)], axis=1)
    pos2 = jnp.concatenate([jnp.sum((p[experts:] + first_total) * hot2[:, b * blk:(b + 1) * blk], axis=0, keepdims=True) for b, p in enumerate(earlier)], axis=1)
    pos1, pos2 = pos1.astype(jnp.int32), pos2.astype(jnp.int32)
    key1 = jnp.where(pos1 < cap, id1 * cap + pos1, -1)
    key2 = jnp.where((pos2 < cap) & (kept2 > 0), id2 * cap + pos2, -1)
    keys[0:1, :] = key1
    keys[1:2, :] = key2

    def x_send(e, k):
        peer = peer_of(me, k)
        return pltpu.make_async_remote_copy(
            src_ref=xs.at[e, pl.ds(pl.multiple_of(peer * cap, cap), cap)],
            dst_ref=xr.at[e, pl.ds(pl.multiple_of(me * cap, cap), cap)],
            send_sem=xs_sem.at[e, k], recv_sem=xr_sem.at[e, k],
            device_id={"ep": peer}, device_id_type=MESH,
        )

    def y_send(e, k):
        peer = peer_of(me, k)
        return pltpu.make_async_remote_copy(
            src_ref=ys.at[e, pl.ds(pl.multiple_of(peer * cap, cap), cap)],
            dst_ref=yr.at[e, pl.ds(pl.multiple_of(me * cap, cap), cap)],
            send_sem=ys_sem.at[e, k], recv_sem=yr_sem.at[e, k],
            device_id={"ep": peer}, device_id_type=MESH,
        )

    mine = pl.ds(pl.multiple_of(me * cap, cap), cap)

    def dispatch(e):
        row = lax.broadcasted_iota(jnp.int32, (rows, tokens), 0)
        slot = (row // cap) * (experts_here * cap) + e * cap + row % cap
        hit = (slot == keys[0:1, :]) | (slot == keys[1:2, :])
        dmat[...] = jnp.where(hit, 1.0, 0.0).astype(bf16)

        def columns(n, _):
            at = pl.ds(pl.multiple_of(n * blk, blk), blk)
            xs[e, :, at] = jnp.dot(dmat[...], tok[:, at], preferred_element_type=f32).astype(bf16)
            return 0

        lax.fori_loop(0, dim // blk, columns, 0)
        xr[e, mine] = xs[e, mine]

    small[2].wait()
    dispatch(0)
    pl.semaphore_wait(barrier, 7)
    for k in SEND_ORDER:
        x_send(0, k).start()

    def dispatch_rest(e, _):
        dispatch(e)
        for k in SEND_ORDER:
            x_send(e, k).start()
        return 0

    lax.fori_loop(1, experts_here, dispatch_rest, 0)

    small[3].wait()
    logits = lax.dot_general(wg[...], tok[...], (((1,), (1,)), ((), ())), preferred_element_type=f32)
    top = jnp.max(logits, axis=0, keepdims=True)
    expd = jnp.exp(logits - top)
    probs = expd / jnp.sum(expd, axis=0, keepdims=True)
    gate1 = jnp.sum(jnp.where(expert_row == ids[0:1, :], probs, 0.0), axis=0, keepdims=True)
    gate2 = jnp.sum(jnp.where((expert_row == ids[1:2, :]) & (keep[0:1, :] > 0), probs, 0.0), axis=0, keepdims=True)
    total = gate1 + gate2
    gates[0:1, :] = keys[0:1, :].astype(f32)
    gates[1:2, :] = keys[1:2, :].astype(f32)
    gates[2:3, :] = gate1 / total
    gates[3:4, :] = gate2 / total
    gates[4:, :] = jnp.zeros((gates.shape[0] - 4, tokens), f32)
    cols[...] = gates[...].T

    def weights(e, _):
        def block(t, _):
            at = pl.ds(pl.multiple_of(t * blk, blk), blk)
            lane = lax.broadcasted_iota(jnp.int32, (blk, rows), 1)
            slot = ((lane // cap) * (experts_here * cap) + e * cap + lane % cap).astype(f32)
            part = cols[at, :]
            cw[e, at, :] = (
                jnp.where(slot == part[:, 0:1], part[:, 2:3], 0.0) + jnp.where(slot == part[:, 1:2], part[:, 3:4], 0.0)
            ).astype(bf16)
            return 0

        return lax.fori_loop(0, tokens // blk, block, 0)

    lax.fori_loop(0, experts_here, weights, 0)

    def expert(e, _):
        s = e % 2
        for k in SEND_ORDER:
            x_send(e, k).wait_recv()
        wi_copy(e).wait()

        def up(j, _):
            at = pl.ds(pl.multiple_of(j * blk, blk), blk)
            pre = jnp.dot(xr[e], wi[s, :, at], preferred_element_type=f32)
            hid[:, at] = jnp.maximum(pre, 0.0).astype(bf16)
            return 0

        lax.fori_loop(0, hidden // blk, up, 0)

        @pl.when(e + 2 < experts_here)
        def _():
            wi_copy(e + 2).start()

        wo_copy(e).wait()

        def down(n, _):
            at = pl.ds(pl.multiple_of(n * blk, blk), blk)
            ys[e, :, at] = jnp.dot(hid[...], wo[s, :, at], preferred_element_type=f32).astype(bf16)
            return 0

        lax.fori_loop(0, dim // blk, down, 0)

        @pl.when(e + 2 < experts_here)
        def _():
            wo_copy(e + 2).start()

        for k in SEND_ORDER:
            y_send(e, k).start()
        yr[e, mine] = ys[e, mine]
        return 0

    lax.fori_loop(0, experts_here, expert, 0)

    def back(e):
        for k in SEND_ORDER:
            y_send(e, k).wait_recv()

    back(0)

    def first_columns(n, _):
        at = pl.ds(pl.multiple_of(n * blk, blk), blk)
        acc[:, at] = jnp.dot(cw[0], yr[0, :, at], preferred_element_type=f32)
        return 0

    lax.fori_loop(0, dim // blk, first_columns, 0)

    def combine(e, _):
        back(e)

        def columns(n, _):
            at = pl.ds(pl.multiple_of(n * blk, blk), blk)
            acc[:, at] += jnp.dot(cw[e], yr[e, :, at], preferred_element_type=f32)
            return 0

        return lax.fori_loop(0, dim // blk, columns, 0)

    lax.fori_loop(1, experts_here - 1, combine, 0)
    last = experts_here - 1
    back(last)

    def finish(t, _):
        at = pl.ds(pl.multiple_of(t * blk, blk), blk)
        obuf[at, :] = (acc[at, :] + jnp.dot(cw[last, at, :], yr[last], preferred_element_type=f32)).astype(bf16)
        return 0

    lax.fori_loop(0, tokens // blk, finish, 0)

    def drain(e, _):
        for k in SEND_ORDER:
            x_send(e, k).wait_send()
            y_send(e, k).wait_send()
        return 0

    lax.fori_loop(0, experts_here, drain, 0)


def solution(mesh):
    def local_layer(tokens, w_gate, expert_ids, keep_second, w_in, w_out):
        _, token_count, dim = tokens.shape
        experts = w_gate.shape[1]
        here, _, hidden = w_in.shape
        cap = 2 * token_count // experts
        groups = experts // here
        rows = groups * cap
        f32, bf16 = jnp.float32, jnp.bfloat16
        vmem, dma = pltpu.VMEM, pltpu.SemaphoreType.DMA
        out = pl.pallas_call(
            functools.partial(layer_kernel, cap),
            out_shape=pltpu.VMEM((token_count, dim), bf16),
            in_specs=[pl.BlockSpec(memory_space=pl.ANY)] * 6,
            out_specs=pl.BlockSpec(memory_space=pltpu.VMEM),
            scratch_shapes=[
                vmem((token_count, dim), bf16),
                vmem((experts, dim), bf16),
                vmem((2, token_count), jnp.int32),
                vmem((1, token_count), jnp.int32),
                vmem((8, token_count), jnp.int32),
                vmem((128, token_count), f32),
                vmem((token_count, 128), f32),
                vmem((rows, token_count), bf16),
                vmem((here, rows, dim), bf16),
                vmem((here, rows, dim), bf16),
                vmem((here, rows, dim), bf16),
                vmem((here, rows, dim), bf16),
                vmem((rows, hidden), bf16),
                vmem((2, dim, hidden), bf16),
                vmem((2, hidden, dim), bf16),
                vmem((here, token_count, rows), bf16),
                vmem((token_count, dim), f32),
                dma((4,)), dma((2,)), dma((2,)),
                dma((here, groups)), dma((here, groups)), dma((here, groups)), dma((here, groups)),
            ],
            compiler_params=pltpu.CompilerParams(collective_id=0, has_side_effects=True, vmem_limit_bytes=60 * 2**20),
            name="moe_layer",
        )(tokens[0], w_gate.T, expert_ids[0].T, keep_second, w_in, w_out)
        return out[None]

    group_spec = P(("dp", "ep"))
    return jax.shard_map(local_layer, mesh=mesh, in_specs=(group_spec, P(), group_spec, group_spec, P("ep"), P("ep")), out_specs=group_spec, check_vma=False)
```

```python
import functools

import jax
import jax.numpy as jnp
from jax import lax
from jax.experimental import pallas as pl
from jax.experimental.pallas import tpu as pltpu
from jax.sharding import PartitionSpec as P

MESH = pl.DeviceIdType.MESH
ORDER = (0, 1, 6, 7, 2, 4, 3, 5)
SENDS = (2, 3, 4, 5, 6, 7, 1)


def peer_of(me, k):
    core, x, y = me % 2, (me // 2) % 2, me // 4
    core_bit, x_bit, y_bit = k % 2, (k // 2) % 2, k // 4
    core = 1 - core if core_bit else core
    x = 1 - x if x_bit else x
    y = 1 - y if y_bit else y
    return (y * 2 + x) * 2 + core


def layer_kernel(
    cap, tok_hbm, wg_hbm, ids_hbm, keep_hbm, win_hbm, wout_hbm, obuf,
    tok, wg, ids, keep, keys, gates, cols, dmat, xs, xr, ys, yr, hid, wi, wo, cw, acc,
    in_sem, wi_sem, wo_sem, xs_sem, xr_sem, ys_sem, yr_sem,
):
    me = lax.axis_index("ep")
    experts_here = win_hbm.shape[0]
    tokens, dim = tok.shape
    experts = wg.shape[0]
    hidden = hid.shape[1]
    groups = experts // experts_here
    rows = groups * cap
    f32, bf16 = jnp.float32, jnp.bfloat16

    small = [
        pltpu.make_async_copy(ids_hbm, ids, in_sem.at[0]),
        pltpu.make_async_copy(keep_hbm, keep, in_sem.at[1]),
        pltpu.make_async_copy(tok_hbm, tok, in_sem.at[2]),
        pltpu.make_async_copy(wg_hbm, wg, in_sem.at[3]),
    ]
    for copy in small:
        copy.start()

    barrier = pltpu.get_barrier_semaphore()
    for k in range(1, 8):
        pl.semaphore_signal(barrier, inc=1, device_id={"ep": peer_of(me, k)}, device_id_type=MESH)

    def wi_copy(e):
        return pltpu.make_async_copy(win_hbm.at[e], wi.at[e % 2], wi_sem.at[e % 2])

    def wo_copy(e):
        return pltpu.make_async_copy(wout_hbm.at[e], wo.at[e % 2], wo_sem.at[e % 2])

    small[0].wait()
    small[1].wait()
    expert_row = lax.broadcasted_iota(jnp.int32, (experts, tokens), 0)
    id1, id2, kept2 = ids[0:1, :], ids[1:2, :], keep[0:1, :]
    hot1 = (expert_row == id1).astype(f32)
    hot2 = ((expert_row == id2) & (kept2 > 0)).astype(f32)
    hot = jnp.concatenate([hot1, hot2], axis=0).astype(bf16)
    blk = 256
    r_io = lax.broadcasted_iota(jnp.int32, (blk, blk), 0)
    c_io = lax.broadcasted_iota(jnp.int32, (blk, blk), 1)
    before = jnp.where(r_io < c_io, 1.0, 0.0).astype(bf16)
    ones = jnp.ones((blk, blk), bf16)
    seen = jnp.zeros((2 * experts, blk), f32)
    earlier = []
    for b in range(tokens // blk):
        part = hot[:, b * blk:(b + 1) * blk]
        earlier.append(jnp.dot(part, before, preferred_element_type=f32) + seen)
        seen = seen + jnp.dot(part, ones, preferred_element_type=f32)
    first_total = seen[:experts, :]
    pos1 = jnp.concatenate([jnp.sum(p[:experts] * hot1[:, b * blk:(b + 1) * blk], axis=0, keepdims=True) for b, p in enumerate(earlier)], axis=1)
    pos2 = jnp.concatenate([jnp.sum((p[experts:] + first_total) * hot2[:, b * blk:(b + 1) * blk], axis=0, keepdims=True) for b, p in enumerate(earlier)], axis=1)
    pos1, pos2 = pos1.astype(jnp.int32), pos2.astype(jnp.int32)
    key1 = jnp.where(pos1 < cap, id1 * cap + pos1, -1)
    key2 = jnp.where((pos2 < cap) & (kept2 > 0), id2 * cap + pos2, -1)
    keys[0:1, :] = key1
    keys[1:2, :] = key2

    def send(src, dst, send_sem, recv_sem, e, p):
        at = pl.ds(p * cap, cap)
        return pltpu.make_async_remote_copy(
            src_ref=src.at[e, at], dst_ref=dst.at[e, at],
            send_sem=send_sem.at[e, p], recv_sem=recv_sem.at[e, p],
            device_id={"ep": peer_of(me, ORDER[p])}, device_id_type=MESH,
        )

    x_send = functools.partial(send, xs, xr, xs_sem, xr_sem)
    y_send = functools.partial(send, ys, yr, ys_sem, yr_sem)

    def first_slot(e, p):
        return peer_of(me, ORDER[p]) * (experts_here * cap) + e * cap

    def pair_hot(e, q):
        row = lax.broadcasted_iota(jnp.int32, (2 * cap, tokens), 0)
        slot = row + jnp.where(row < cap, first_slot(e, 2 * q), first_slot(e, 2 * q + 1) - cap)
        hit = (slot == keys[0:1, :]) | (slot == keys[1:2, :])
        return jnp.where(hit, 1.0, 0.0).astype(bf16)

    small[2].wait()
    for q in (1, 2, 3, 0):
        at = pl.ds(q * 2 * cap, 2 * cap)
        xs[0, at] = jnp.dot(pair_hot(0, q), tok[...], preferred_element_type=f32).astype(bf16)
        if q == 1:
            pl.semaphore_wait(barrier, 7)
        for p in (2 * q, 2 * q + 1):
            if p:
                x_send(0, p).start()
    xr[0, 0:cap] = xs[0, 0:cap]
    for e in range(2):
        wi_copy(e).start()
        wo_copy(e).start()

    def dispatch(e, _):
        for q in range(groups // 2):
            dmat[pl.ds(q * 2 * cap, 2 * cap), :] = pair_hot(e, q)

        def columns(n, _):
            at = pl.ds(pl.multiple_of(n * blk, blk), blk)
            xs[e, :, at] = jnp.dot(dmat[...], tok[:, at], preferred_element_type=f32).astype(bf16)
            return 0

        lax.fori_loop(0, dim // blk, columns, 0)
        for p in SENDS:
            x_send(e, p).start()
        xr[e, 0:cap] = xs[e, 0:cap]
        return 0

    lax.fori_loop(1, experts_here, dispatch, 0)

    small[3].wait()
    logits = lax.dot_general(wg[...], tok[...], (((1,), (1,)), ((), ())), preferred_element_type=f32)
    top = jnp.max(logits, axis=0, keepdims=True)
    expd = jnp.exp(logits - top)
    probs = expd / jnp.sum(expd, axis=0, keepdims=True)
    gate1 = jnp.sum(jnp.where(expert_row == ids[0:1, :], probs, 0.0), axis=0, keepdims=True)
    gate2 = jnp.sum(jnp.where((expert_row == ids[1:2, :]) & (keep[0:1, :] > 0), probs, 0.0), axis=0, keepdims=True)
    total = gate1 + gate2
    gates[0:1, :] = keys[0:1, :].astype(f32)
    gates[1:2, :] = keys[1:2, :].astype(f32)
    gates[2:3, :] = gate1 / total
    gates[3:4, :] = gate2 / total
    gates[4:, :] = jnp.zeros((gates.shape[0] - 4, tokens), f32)
    cols[...] = gates[...].T

    def weights(e, _):
        def block(t, _):
            at = pl.ds(pl.multiple_of(t * blk, blk), blk)
            lane = lax.broadcasted_iota(jnp.int32, (8, rows), 1)
            slot = lane
            for p in range(groups):
                slot = slot + jnp.where(lane // cap == p, first_slot(e, p) - p * cap, 0)
            slot = slot[0:1, :].astype(f32)
            part = cols[at, :]
            cw[e, at, :] = (
                jnp.where(slot == part[:, 0:1], part[:, 2:3], 0.0) + jnp.where(slot == part[:, 1:2], part[:, 3:4], 0.0)
            ).astype(bf16)
            return 0

        return lax.fori_loop(0, tokens // blk, block, 0)

    lax.fori_loop(0, experts_here, weights, 0)

    def expert(e, _):
        s = e % 2
        for p in SENDS:
            x_send(e, p).wait_recv()
        wi_copy(e).wait()

        def up(j, _):
            at = pl.ds(pl.multiple_of(j * blk, blk), blk)
            pre = jnp.dot(xr[e], wi[s, :, at], preferred_element_type=f32)
            hid[:, at] = jnp.maximum(pre, 0.0).astype(bf16)
            return 0

        lax.fori_loop(0, hidden // blk, up, 0)

        @pl.when(e + 2 < experts_here)
        def _():
            wi_copy(e + 2).start()

        wo_copy(e).wait()

        def down(n, _):
            at = pl.ds(pl.multiple_of(n * blk, blk), blk)
            ys[e, :, at] = jnp.dot(hid[...], wo[s, :, at], preferred_element_type=f32).astype(bf16)
            return 0

        lax.fori_loop(0, dim // blk, down, 0)

        @pl.when(e + 2 < experts_here)
        def _():
            wo_copy(e + 2).start()

        for p in SENDS:
            y_send(e, p).start()
        yr[e, 0:cap] = ys[e, 0:cap]
        return 0

    lax.fori_loop(0, experts_here, expert, 0)

    def first_columns(n, _):
        at = pl.ds(pl.multiple_of(n * blk, blk), blk)
        acc[:, at] = jnp.dot(cw[0], yr[0, :, at], preferred_element_type=f32)
        return 0

    def combine(e, _):
        for p in SENDS:
            y_send(e, p).wait_recv()

        def columns(n, _):
            at = pl.ds(pl.multiple_of(n * blk, blk), blk)
            acc[:, at] += jnp.dot(cw[e], yr[e, :, at], preferred_element_type=f32)
            return 0

        return lax.fori_loop(0, dim // blk, columns, 0)

    for p in SENDS:
        y_send(0, p).wait_recv()
    lax.fori_loop(0, dim // blk, first_columns, 0)
    lax.fori_loop(1, experts_here - 1, combine, 0)
    last = experts_here - 1
    for q in range(groups // 2 - 1):
        for p in (2 * q, 2 * q + 1):
            if p:
                y_send(last, p).wait_recv()
        pair = pl.ds(q * 2 * cap, 2 * cap)

        def pair_columns(n, _):
            at = pl.ds(pl.multiple_of(n * blk, blk), blk)
            acc[:, at] += jnp.dot(cw[last, :, pair], yr[last, pair, at], preferred_element_type=f32)
            return 0

        lax.fori_loop(0, dim // blk, pair_columns, 0)
    for p in (groups - 2, groups - 1):
        y_send(last, p).wait_recv()
    pair = pl.ds(rows - 2 * cap, 2 * cap)
    for t in range(tokens // blk):
        at = pl.ds(t * blk, blk)
        obuf[at, :] = (acc[at, :] + jnp.dot(cw[last, at, pair], yr[last, pair], preferred_element_type=f32)).astype(bf16)

    def drain(e, _):
        for p in SENDS:
            x_send(e, p).wait_send()
            y_send(e, p).wait_send()
        return 0

    lax.fori_loop(0, experts_here, drain, 0)


def solution(mesh):
    def local_layer(tokens, w_gate, expert_ids, keep_second, w_in, w_out):
        _, token_count, dim = tokens.shape
        experts = w_gate.shape[1]
        here, _, hidden = w_in.shape
        cap = 2 * token_count // experts
        groups = experts // here
        rows = groups * cap
        f32, bf16 = jnp.float32, jnp.bfloat16
        vmem, dma = pltpu.VMEM, pltpu.SemaphoreType.DMA
        out = pl.pallas_call(
            functools.partial(layer_kernel, cap),
            out_shape=pltpu.VMEM((token_count, dim), bf16),
            in_specs=[pl.BlockSpec(memory_space=pl.ANY)] * 6,
            out_specs=pl.BlockSpec(memory_space=pltpu.VMEM),
            scratch_shapes=[
                vmem((token_count, dim), bf16),
                vmem((experts, dim), bf16),
                vmem((2, token_count), jnp.int32),
                vmem((1, token_count), jnp.int32),
                vmem((8, token_count), jnp.int32),
                vmem((128, token_count), f32),
                vmem((token_count, 128), f32),
                vmem((rows, token_count), bf16),
                vmem((here, rows, dim), bf16),
                vmem((here, rows, dim), bf16),
                vmem((here, rows, dim), bf16),
                vmem((here, rows, dim), bf16),
                vmem((rows, hidden), bf16),
                vmem((2, dim, hidden), bf16),
                vmem((2, hidden, dim), bf16),
                vmem((here, token_count, rows), bf16),
                vmem((token_count, dim), f32),
                dma((4,)), dma((2,)), dma((2,)),
                dma((here, groups)), dma((here, groups)), dma((here, groups)), dma((here, groups)),
            ],
            compiler_params=pltpu.CompilerParams(collective_id=0, has_side_effects=True, vmem_limit_bytes=60 * 2**20),
            name="moe_layer",
        )(tokens[0], w_gate.T, expert_ids[0].T, keep_second, w_in, w_out)
        return out[None]

    group_spec = P(("dp", "ep"))
    return jax.shard_map(local_layer, mesh=mesh, in_specs=(group_spec, P(), group_spec, group_spec, P("ep"), P("ep")), out_specs=group_spec, check_vma=False)
```

```python
import functools

import jax
import jax.numpy as jnp
from jax import lax
from jax.experimental import pallas as pl
from jax.experimental.pallas import tpu as pltpu
from jax.sharding import PartitionSpec as P

MESH = pl.DeviceIdType.MESH
ORDER = (0, 1, 6, 7, 2, 4, 3, 5)
SENDS = (2, 3, 4, 5, 6, 7, 1)
X_PIECES = ((0, 1), (1, 1), (2, 2))
Y_PIECES = ((0, 2), (2, 1), (3, 1))


def peer_of(me, k):
    core, x, y = me % 2, (me // 2) % 2, me // 4
    core_bit, x_bit, y_bit = k % 2, (k // 2) % 2, k // 4
    core = 1 - core if core_bit else core
    x = 1 - x if x_bit else x
    y = 1 - y if y_bit else y
    return (y * 2 + x) * 2 + core


def layer_kernel(
    cap, tok_hbm, wg_hbm, ids_hbm, keep_hbm, win_hbm, wout_hbm, acc, cw_end, y_end,
    tok, wg, ids, keep, keys, gates, cols, dmat, xs, xr, ys, yr, hid, wi, wo, cw,
    in_sem, wi_sem, wo_sem, xs_sem, xr_sem, ys_sem, yr_sem,
):
    me = lax.axis_index("ep")
    experts_here = win_hbm.shape[0]
    tokens, dim = tok.shape
    experts = wg.shape[0]
    hidden = hid.shape[1]
    groups = experts // experts_here
    rows = groups * cap
    f32, bf16 = jnp.float32, jnp.bfloat16

    small = [
        pltpu.make_async_copy(ids_hbm, ids, in_sem.at[0]),
        pltpu.make_async_copy(keep_hbm, keep, in_sem.at[1]),
        pltpu.make_async_copy(tok_hbm, tok, in_sem.at[2]),
        pltpu.make_async_copy(wg_hbm, wg, in_sem.at[3]),
    ]
    for copy in small:
        copy.start()

    barrier = pltpu.get_barrier_semaphore()
    for k in range(1, 8):
        pl.semaphore_signal(barrier, inc=1, device_id={"ep": peer_of(me, k)}, device_id_type=MESH)

    def wi_copy(e):
        return pltpu.make_async_copy(win_hbm.at[e], wi.at[e % 2], wi_sem.at[e % 2])

    def wo_copy(e):
        return pltpu.make_async_copy(wout_hbm.at[e], wo.at[e % 2], wo_sem.at[e % 2])

    small[0].wait()
    small[1].wait()
    expert_row = lax.broadcasted_iota(jnp.int32, (experts, tokens), 0)
    id1, id2, kept2 = ids[0:1, :], ids[1:2, :], keep[0:1, :]
    hot1 = (expert_row == id1).astype(f32)
    hot2 = ((expert_row == id2) & (kept2 > 0)).astype(f32)
    hot = jnp.concatenate([hot1, hot2], axis=0).astype(bf16)
    blk = 256
    r_io = lax.broadcasted_iota(jnp.int32, (blk, blk), 0)
    c_io = lax.broadcasted_iota(jnp.int32, (blk, blk), 1)
    before = jnp.where(r_io < c_io, 1.0, 0.0).astype(bf16)
    ones = jnp.ones((blk, blk), bf16)
    seen = jnp.zeros((2 * experts, blk), f32)
    earlier = []
    for b in range(tokens // blk):
        part = hot[:, b * blk:(b + 1) * blk]
        earlier.append(jnp.dot(part, before, preferred_element_type=f32) + seen)
        seen = seen + jnp.dot(part, ones, preferred_element_type=f32)
    first_total = seen[:experts, :]
    pos1 = jnp.concatenate([jnp.sum(p[:experts] * hot1[:, b * blk:(b + 1) * blk], axis=0, keepdims=True) for b, p in enumerate(earlier)], axis=1)
    pos2 = jnp.concatenate([jnp.sum((p[experts:] + first_total) * hot2[:, b * blk:(b + 1) * blk], axis=0, keepdims=True) for b, p in enumerate(earlier)], axis=1)
    pos1, pos2 = pos1.astype(jnp.int32), pos2.astype(jnp.int32)
    key1 = jnp.where(pos1 < cap, id1 * cap + pos1, -1)
    key2 = jnp.where((pos2 < cap) & (kept2 > 0), id2 * cap + pos2, -1)
    keys[0:1, :] = key1
    keys[1:2, :] = key2

    def send(src, dst, send_sem, recv_sem, pieces, i, p):
        at = pl.ds(*pieces[i])
        return pltpu.make_async_remote_copy(
            src_ref=src.at[p, at], dst_ref=dst.at[p, at],
            send_sem=send_sem.at[i, p], recv_sem=recv_sem.at[i, p],
            device_id={"ep": peer_of(me, ORDER[p])}, device_id_type=MESH,
        )

    x_send = functools.partial(send, xs, xr, xs_sem, xr_sem, X_PIECES)
    y_send = functools.partial(send, ys, yr, ys_sem, yr_sem, Y_PIECES)

    def first_slot(e, p):
        return peer_of(me, ORDER[p]) * (experts_here * cap) + e * cap

    def pair_hot(e, q):
        row = lax.broadcasted_iota(jnp.int32, (2 * cap, tokens), 0)
        slot = row + jnp.where(row < cap, first_slot(e, 2 * q), first_slot(e, 2 * q + 1) - cap)
        hit = (slot == keys[0:1, :]) | (slot == keys[1:2, :])
        return jnp.where(hit, 1.0, 0.0).astype(bf16)

    small[2].wait()
    for q in (1, 2, 3, 0):
        got = jnp.dot(pair_hot(0, q), tok[...], preferred_element_type=f32).astype(bf16)
        for p, part in ((2 * q, got[:cap]), (2 * q + 1, got[cap:])):
            if p:
                xs[p, 0] = part
            else:
                xr[p, 0] = part
        if q == 1:
            pl.semaphore_wait(barrier, 7)
        for p in (2 * q, 2 * q + 1):
            if p:
                x_send(0, p).start()
    for e in range(2):
        wi_copy(e).start()
        wo_copy(e).start()

    def dispatch(e, _):
        for q in range(groups // 2):
            dmat[pl.ds(q * 2 * cap, 2 * cap), :] = pair_hot(e, q)

        def columns(n, _):
            at = pl.ds(pl.multiple_of(n * blk, blk), blk)
            got = jnp.dot(dmat[...], tok[:, at], preferred_element_type=f32).astype(bf16)
            xs[:, e, :, at] = got.reshape(groups, cap, blk)
            return 0

        lax.fori_loop(0, dim // blk, columns, 0)
        for i, (start, count) in enumerate(X_PIECES[1:], 1):
            @pl.when(e == start + count - 1)
            def _():
                for p in SENDS:
                    x_send(i, p).start()
        xr[0, e] = xs[0, e]
        return 0

    lax.fori_loop(1, experts_here, dispatch, 0)

    small[3].wait()
    logits = lax.dot_general(wg[...], tok[...], (((1,), (1,)), ((), ())), preferred_element_type=f32)
    top = jnp.max(logits, axis=0, keepdims=True)
    expd = jnp.exp(logits - top)
    probs = expd / jnp.sum(expd, axis=0, keepdims=True)
    gate1 = jnp.sum(jnp.where(expert_row == ids[0:1, :], probs, 0.0), axis=0, keepdims=True)
    gate2 = jnp.sum(jnp.where((expert_row == ids[1:2, :]) & (keep[0:1, :] > 0), probs, 0.0), axis=0, keepdims=True)
    total = gate1 + gate2
    gates[0:1, :] = keys[0:1, :].astype(f32)
    gates[1:2, :] = keys[1:2, :].astype(f32)
    gates[2:3, :] = gate1 / total
    gates[3:4, :] = gate2 / total
    gates[4:, :] = jnp.zeros((gates.shape[0] - 4, tokens), f32)
    cols[...] = gates[...].T

    def weights(e, _):
        def block(t, _):
            at = pl.ds(pl.multiple_of(t * blk, blk), blk)
            lane = lax.broadcasted_iota(jnp.int32, (8, rows), 1)
            slot = lane
            for p in range(groups):
                slot = slot + jnp.where(lane // cap == p, first_slot(e, p) - p * cap, 0)
            slot = slot[0:1, :].astype(f32)
            part = cols[at, :]
            cw[e, at, :] = (
                jnp.where(slot == part[:, 0:1], part[:, 2:3], 0.0) + jnp.where(slot == part[:, 1:2], part[:, 3:4], 0.0)
            ).astype(bf16)
            return 0

        return lax.fori_loop(0, tokens // blk, block, 0)

    lax.fori_loop(0, experts_here, weights, 0)

    def expert(e, _):
        s = e % 2
        for i, (start, _count) in enumerate(X_PIECES):
            @pl.when(e == start)
            def _():
                for p in SENDS:
                    x_send(i, p).wait_recv()

        wi_copy(e).wait()

        def up(j, _):
            at = pl.ds(pl.multiple_of(j * blk, blk), blk)
            pre = jnp.dot(xr[:, e].reshape(rows, dim), wi[s, :, at], preferred_element_type=f32)
            hid[:, at] = jnp.maximum(pre, 0.0).astype(bf16)
            return 0

        lax.fori_loop(0, hidden // blk, up, 0)

        @pl.when(e + 2 < experts_here)
        def _():
            wi_copy(e + 2).start()

        wo_copy(e).wait()

        def down(n, _):
            at = pl.ds(pl.multiple_of(n * blk, blk), blk)
            got = jnp.dot(hid[...], wo[s, :, at], preferred_element_type=f32).astype(bf16)
            ys[:, e, :, at] = got.reshape(groups, cap, blk)
            return 0

        lax.fori_loop(0, dim // blk, down, 0)

        @pl.when(e + 2 < experts_here)
        def _():
            wo_copy(e + 2).start()

        for i, (start, count) in enumerate(Y_PIECES):
            @pl.when(e == start + count - 1)
            def _():
                for p in SENDS:
                    y_send(i, p).start()
        yr[0, e] = ys[0, e]
        return 0

    lax.fori_loop(0, experts_here, expert, 0)

    def first_columns(n, _):
        at = pl.ds(pl.multiple_of(n * blk, blk), blk)
        acc[:, at] = jnp.dot(cw[0], yr[:, 0, :, at].reshape(rows, blk), preferred_element_type=f32)
        return 0

    def combine(e, _):
        @pl.when(e == Y_PIECES[1][0])
        def _():
            for p in SENDS:
                y_send(1, p).wait_recv()

        def columns(n, _):
            at = pl.ds(pl.multiple_of(n * blk, blk), blk)
            acc[:, at] += jnp.dot(cw[e], yr[:, e, :, at].reshape(rows, blk), preferred_element_type=f32)
            return 0

        return lax.fori_loop(0, dim // blk, columns, 0)

    for p in SENDS:
        y_send(0, p).wait_recv()
    lax.fori_loop(0, dim // blk, first_columns, 0)
    lax.fori_loop(1, experts_here - 1, combine, 0)
    last = experts_here - 1
    for q in range(groups // 2 - 1):
        for p in (2 * q, 2 * q + 1):
            if p:
                y_send(2, p).wait_recv()
        pair = pl.ds(q * 2 * cap, 2 * cap)

        def pair_columns(n, _):
            at = pl.ds(pl.multiple_of(n * blk, blk), blk)
            back = yr[2 * q:2 * q + 2, last, :, at].reshape(2 * cap, blk)
            acc[:, at] += jnp.dot(cw[last, :, pair], back, preferred_element_type=f32)
            return 0

        lax.fori_loop(0, dim // blk, pair_columns, 0)
    pair = pl.ds(rows - 2 * cap, 2 * cap)
    cw_end[...] = cw[last, :, pair]
    for p in (groups - 2, groups - 1):
        y_send(2, p).wait_recv()
    y_end[...] = yr[groups - 2:, last].reshape(2 * cap, dim)

    for i in range(len(X_PIECES)):
        for p in SENDS:
            x_send(i, p).wait_send()
            y_send(i, p).wait_send()


def finish_kernel(acc, cw, y, out, buf, sem):
    blk = buf.shape[0] // 4
    copies = []
    for t in range(4):
        at = pl.ds(t * blk, blk)
        buf[at, :] = (acc[at, :] + jnp.dot(cw[at, :], y[...], preferred_element_type=jnp.float32)).astype(out.dtype)
        copies.append(pltpu.make_async_copy(buf.at[at], out.at[at], sem.at[t]))
        copies[-1].start()
    for copy in copies:
        copy.wait()


def solution(mesh):
    def local_layer(tokens, w_gate, expert_ids, keep_second, w_in, w_out):
        _, token_count, dim = tokens.shape
        experts = w_gate.shape[1]
        here, _, hidden = w_in.shape
        cap = 2 * token_count // experts
        groups = experts // here
        rows = groups * cap
        f32, bf16 = jnp.float32, jnp.bfloat16
        vmem, dma = pltpu.VMEM, pltpu.SemaphoreType.DMA
        acc, cw_end, y_end = pl.pallas_call(
            functools.partial(layer_kernel, cap),
            out_shape=(vmem((token_count, dim), f32), vmem((token_count, 2 * cap), bf16), vmem((2 * cap, dim), bf16)),
            in_specs=[pl.BlockSpec(memory_space=pl.ANY)] * 6,
            out_specs=[pl.BlockSpec(memory_space=vmem)] * 3,
            scratch_shapes=[
                vmem((token_count, dim), bf16),
                vmem((experts, dim), bf16),
                vmem((2, token_count), jnp.int32),
                vmem((1, token_count), jnp.int32),
                vmem((8, token_count), jnp.int32),
                vmem((128, token_count), f32),
                vmem((token_count, 128), f32),
                vmem((rows, token_count), bf16),
                vmem((groups, here, cap, dim), bf16),
                vmem((groups, here, cap, dim), bf16),
                vmem((groups, here, cap, dim), bf16),
                vmem((groups, here, cap, dim), bf16),
                vmem((rows, hidden), bf16),
                vmem((2, dim, hidden), bf16),
                vmem((2, hidden, dim), bf16),
                vmem((here, token_count, rows), bf16),
                dma((4,)), dma((2,)), dma((2,)),
                dma((3, groups)), dma((3, groups)), dma((3, groups)), dma((3, groups)),
            ],
            compiler_params=pltpu.CompilerParams(collective_id=0, has_side_effects=True, vmem_limit_bytes=56 * 2**20),
            name="moe_layer",
        )(tokens[0], w_gate.T, expert_ids[0].T, keep_second, w_in, w_out)
        out = pl.pallas_call(
            finish_kernel,
            out_shape=jax.ShapeDtypeStruct((token_count, dim), bf16),
            in_specs=[pl.BlockSpec(memory_space=vmem)] * 3,
            out_specs=pl.BlockSpec(memory_space=pl.ANY),
            scratch_shapes=[vmem((token_count, dim), bf16), dma((4,))],
            compiler_params=pltpu.CompilerParams(vmem_limit_bytes=8 * 2**20),
            name="moe_finish",
        )(acc, cw_end, y_end)
        return out[None]

    group_spec = P(("dp", "ep"))
    return jax.shard_map(local_layer, mesh=mesh, in_specs=(group_spec, P(), group_spec, group_spec, P("ep"), P("ep")), out_specs=group_spec, check_vma=False)
```

```python
import functools

import jax
import jax.numpy as jnp
from jax import lax
from jax.experimental import pallas as pl
from jax.experimental.pallas import tpu as pltpu
from jax.sharding import PartitionSpec as P

MESH = pl.DeviceIdType.MESH
ORDER = (0, 1, 6, 7, 2, 4, 3, 5)
SENDS = (2, 3, 4, 5, 6, 7, 1)
X_PIECES = ((0, 1), (1, 1), (2, 2))
Y_PIECES = ((0, 2), (2, 2))


def peer_of(me, k):
    core, x, y = me % 2, (me // 2) % 2, me // 4
    core_bit, x_bit, y_bit = k % 2, (k // 2) % 2, k // 4
    core = 1 - core if core_bit else core
    x = 1 - x if x_bit else x
    y = 1 - y if y_bit else y
    return (y * 2 + x) * 2 + core


def layer_kernel(
    cap, tok_hbm, wg_hbm, ids_hbm, keep_hbm, win_hbm, wout_hbm, acc, cw_end, y_end,
    tok, wg, ids, keep, keys, gates, cols, dmat, xs, xr, ys, yr, hid, wi, wo, cw,
    in_sem, wi_sem, wo_sem, xs_sem, xr_sem, ys_sem, yr_sem,
):
    me = lax.axis_index("ep")
    experts_here = win_hbm.shape[0]
    tokens, dim = tok.shape
    experts = wg.shape[0]
    hidden = hid.shape[1]
    groups = experts // experts_here
    rows = groups * cap
    f32, bf16 = jnp.float32, jnp.bfloat16

    small = [
        pltpu.make_async_copy(ids_hbm, ids, in_sem.at[0]),
        pltpu.make_async_copy(keep_hbm, keep, in_sem.at[1]),
        pltpu.make_async_copy(tok_hbm, tok, in_sem.at[2]),
        pltpu.make_async_copy(wg_hbm, wg, in_sem.at[3]),
    ]
    for copy in small:
        copy.start()

    barrier = pltpu.get_barrier_semaphore()
    for k in range(1, 8):
        pl.semaphore_signal(barrier, inc=1, device_id={"ep": peer_of(me, k)}, device_id_type=MESH)

    def wi_copy(e):
        return pltpu.make_async_copy(win_hbm.at[e], wi.at[e % 2], wi_sem.at[e % 2])

    def wo_copy(e):
        return pltpu.make_async_copy(wout_hbm.at[e], wo.at[e % 2], wo_sem.at[e % 2])

    small[0].wait()
    small[1].wait()
    expert_row = lax.broadcasted_iota(jnp.int32, (experts, tokens), 0)
    id1, id2, kept2 = ids[0:1, :], ids[1:2, :], keep[0:1, :]
    hot1 = (expert_row == id1).astype(f32)
    hot2 = ((expert_row == id2) & (kept2 > 0)).astype(f32)
    hot = jnp.concatenate([hot1, hot2], axis=0).astype(bf16)
    blk = 256
    r_io = lax.broadcasted_iota(jnp.int32, (blk, blk), 0)
    c_io = lax.broadcasted_iota(jnp.int32, (blk, blk), 1)
    before = jnp.where(r_io < c_io, 1.0, 0.0).astype(bf16)
    ones = jnp.ones((blk, blk), bf16)
    seen = jnp.zeros((2 * experts, blk), f32)
    earlier = []
    for b in range(tokens // blk):
        part = hot[:, b * blk:(b + 1) * blk]
        earlier.append(jnp.dot(part, before, preferred_element_type=f32) + seen)
        seen = seen + jnp.dot(part, ones, preferred_element_type=f32)
    first_total = seen[:experts, :]
    pos1 = jnp.concatenate([jnp.sum(p[:experts] * hot1[:, b * blk:(b + 1) * blk], axis=0, keepdims=True) for b, p in enumerate(earlier)], axis=1)
    pos2 = jnp.concatenate([jnp.sum((p[experts:] + first_total) * hot2[:, b * blk:(b + 1) * blk], axis=0, keepdims=True) for b, p in enumerate(earlier)], axis=1)
    pos1, pos2 = pos1.astype(jnp.int32), pos2.astype(jnp.int32)
    key1 = jnp.where(pos1 < cap, id1 * cap + pos1, -1)
    key2 = jnp.where((pos2 < cap) & (kept2 > 0), id2 * cap + pos2, -1)
    keys[0:1, :] = key1
    keys[1:2, :] = key2

    def send(src, dst, send_sem, recv_sem, pieces, i, p):
        at = pl.ds(*pieces[i])
        return pltpu.make_async_remote_copy(
            src_ref=src.at[p, at], dst_ref=dst.at[p, at],
            send_sem=send_sem.at[i, p], recv_sem=recv_sem.at[i, p],
            device_id={"ep": peer_of(me, ORDER[p])}, device_id_type=MESH,
        )

    x_send = functools.partial(send, xs, xr, xs_sem, xr_sem, X_PIECES)
    y_send = functools.partial(send, ys, yr, ys_sem, yr_sem, Y_PIECES)

    def first_slot(e, p):
        return peer_of(me, ORDER[p]) * (experts_here * cap) + e * cap

    def pair_hot(e, q):
        row = lax.broadcasted_iota(jnp.int32, (2 * cap, tokens), 0)
        slot = row + jnp.where(row < cap, first_slot(e, 2 * q), first_slot(e, 2 * q + 1) - cap)
        hit = (slot == keys[0:1, :]) | (slot == keys[1:2, :])
        return jnp.where(hit, 1.0, 0.0).astype(bf16)

    small[2].wait()
    for half in ((1, 2), (3, 0)):
        for i, q in enumerate(half):
            dmat[pl.ds(i * 2 * cap, 2 * cap), :] = pair_hot(0, q)
        got = jnp.dot(dmat[0:4 * cap, :], tok[...], preferred_element_type=f32).astype(bf16)
        blocks = [2 * q + side for q in half for side in (0, 1)]
        for i, p in enumerate(blocks):
            if p:
                xs[p, 0] = got[i * cap:(i + 1) * cap]
            else:
                xr[p, 0] = got[i * cap:(i + 1) * cap]
        if half[0] == 1:
            pl.semaphore_wait(barrier, 7)
        for p in blocks:
            if p:
                x_send(0, p).start()
    for e in range(2):
        wi_copy(e).start()
        wo_copy(e).start()

    def dispatch(e, _):
        for q in range(groups // 2):
            dmat[pl.ds(q * 2 * cap, 2 * cap), :] = pair_hot(e, q)

        def columns(n, _):
            at = pl.ds(pl.multiple_of(n * blk, blk), blk)
            got = jnp.dot(dmat[...], tok[:, at], preferred_element_type=f32).astype(bf16)
            xs[:, e, :, at] = got.reshape(groups, cap, blk)
            return 0

        lax.fori_loop(0, dim // blk, columns, 0)
        for i, (start, count) in enumerate(X_PIECES[1:], 1):
            @pl.when(e == start + count - 1)
            def _():
                for p in SENDS:
                    x_send(i, p).start()
        xr[0, e] = xs[0, e]
        return 0

    lax.fori_loop(1, experts_here, dispatch, 0)

    small[3].wait()
    logits = lax.dot_general(wg[...], tok[...], (((1,), (1,)), ((), ())), preferred_element_type=f32)
    top = jnp.max(logits, axis=0, keepdims=True)
    expd = jnp.exp(logits - top)
    probs = expd / jnp.sum(expd, axis=0, keepdims=True)
    gate1 = jnp.sum(jnp.where(expert_row == ids[0:1, :], probs, 0.0), axis=0, keepdims=True)
    gate2 = jnp.sum(jnp.where((expert_row == ids[1:2, :]) & (keep[0:1, :] > 0), probs, 0.0), axis=0, keepdims=True)
    total = gate1 + gate2
    gates[0:1, :] = keys[0:1, :].astype(f32)
    gates[1:2, :] = keys[1:2, :].astype(f32)
    gates[2:3, :] = gate1 / total
    gates[3:4, :] = gate2 / total
    gates[4:, :] = jnp.zeros((gates.shape[0] - 4, tokens), f32)
    cols[...] = gates[...].T

    def weights(i, _):
        def block(t, _):
            at = pl.ds(pl.multiple_of(t * blk, blk), blk)
            lane = lax.broadcasted_iota(jnp.int32, (8, 2 * rows), 1)
            slot = lane
            for p in range(groups):
                slot = slot + jnp.where(lane // (2 * cap) == p, first_slot(2 * i, p) - p * 2 * cap, 0)
            slot = slot[0:1, :].astype(f32)
            part = cols[at, :]
            cw[i, at, :] = (
                jnp.where(slot == part[:, 0:1], part[:, 2:3], 0.0) + jnp.where(slot == part[:, 1:2], part[:, 3:4], 0.0)
            ).astype(bf16)
            return 0

        return lax.fori_loop(0, tokens // blk, block, 0)

    lax.fori_loop(0, experts_here // 2, weights, 0)

    def expert(e, _):
        s = e % 2
        for i, (start, _count) in enumerate(X_PIECES):
            @pl.when(e == start)
            def _():
                for p in SENDS:
                    x_send(i, p).wait_recv()

        wi_copy(e).wait()

        def up(j, _):
            at = pl.ds(pl.multiple_of(j * blk, blk), blk)
            pre = jnp.dot(xr[:, e].reshape(rows, dim), wi[s, :, at], preferred_element_type=f32)
            hid[:, at] = jnp.maximum(pre, 0.0).astype(bf16)
            return 0

        lax.fori_loop(0, hidden // blk, up, 0)

        @pl.when(e + 2 < experts_here)
        def _():
            wi_copy(e + 2).start()

        wo_copy(e).wait()

        def down(n, _):
            at = pl.ds(pl.multiple_of(n * blk, blk), blk)
            got = jnp.dot(hid[...], wo[s, :, at], preferred_element_type=f32).astype(bf16)
            ys[:, e, :, at] = got.reshape(groups, cap, blk)
            return 0

        lax.fori_loop(0, dim // blk, down, 0)

        @pl.when(e + 2 < experts_here)
        def _():
            wo_copy(e + 2).start()

        for i, (start, count) in enumerate(Y_PIECES):
            @pl.when(e == start + count - 1)
            def _():
                for p in SENDS:
                    y_send(i, p).start()
        yr[0, e] = ys[0, e]
        return 0

    lax.fori_loop(0, experts_here, expert, 0)

    for p in SENDS:
        y_send(0, p).wait_recv()

    def columns(n, _):
        at = pl.ds(pl.multiple_of(n * blk, blk), blk)
        acc[:, at] = jnp.dot(cw[0], yr[:, 0:2, :, at].reshape(2 * rows, blk), preferred_element_type=f32)
        return 0

    lax.fori_loop(0, dim // blk, columns, 0)
    for q in range(groups // 2 - 1):
        for p in (2 * q, 2 * q + 1):
            if p:
                y_send(1, p).wait_recv()

        def pair_columns(n, _):
            at = pl.ds(pl.multiple_of(n * blk, blk), blk)
            back = yr[2 * q:2 * q + 2, 2:4, :, at].reshape(4 * cap, blk)
            acc[:, at] += jnp.dot(cw[1, :, q * 4 * cap:(q + 1) * 4 * cap], back, preferred_element_type=f32)
            return 0

        lax.fori_loop(0, dim // blk, pair_columns, 0)
    cw_end[...] = cw[1, :, 2 * rows - 4 * cap:]
    for p in (groups - 2, groups - 1):
        y_send(1, p).wait_recv()
    y_end[...] = yr[groups - 2:, 2:4].reshape(4 * cap, dim)

    for i in range(len(X_PIECES)):
        for p in SENDS:
            x_send(i, p).wait_send()
    for i in range(len(Y_PIECES)):
        for p in SENDS:
            y_send(i, p).wait_send()


def finish_kernel(acc, cw, y, out, buf, sem):
    blk = buf.shape[0] // 8
    copies = []
    for t in range(8):
        at = pl.ds(t * blk, blk)
        buf[at, :] = (acc[at, :] + jnp.dot(cw[at, :], y[...], preferred_element_type=jnp.float32)).astype(out.dtype)
        copies.append(pltpu.make_async_copy(buf.at[at], out.at[at], sem.at[t]))
        copies[-1].start()
    for copy in copies:
        copy.wait()


def solution(mesh):
    def local_layer(tokens, w_gate, expert_ids, keep_second, w_in, w_out):
        _, token_count, dim = tokens.shape
        experts = w_gate.shape[1]
        here, _, hidden = w_in.shape
        cap = 2 * token_count // experts
        groups = experts // here
        rows = groups * cap
        f32, bf16 = jnp.float32, jnp.bfloat16
        vmem, dma = pltpu.VMEM, pltpu.SemaphoreType.DMA
        acc, cw_end, y_end = pl.pallas_call(
            functools.partial(layer_kernel, cap),
            out_shape=(vmem((token_count, dim), f32), vmem((token_count, 4 * cap), bf16), vmem((4 * cap, dim), bf16)),
            in_specs=[pl.BlockSpec(memory_space=pl.ANY)] * 6,
            out_specs=[pl.BlockSpec(memory_space=vmem)] * 3,
            scratch_shapes=[
                vmem((token_count, dim), bf16),
                vmem((experts, dim), bf16),
                vmem((2, token_count), jnp.int32),
                vmem((1, token_count), jnp.int32),
                vmem((8, token_count), jnp.int32),
                vmem((128, token_count), f32),
                vmem((token_count, 128), f32),
                vmem((rows, token_count), bf16),
                vmem((groups, here, cap, dim), bf16),
                vmem((groups, here, cap, dim), bf16),
                vmem((groups, here, cap, dim), bf16),
                vmem((groups, here, cap, dim), bf16),
                vmem((rows, hidden), bf16),
                vmem((2, dim, hidden), bf16),
                vmem((2, hidden, dim), bf16),
                vmem((here // 2, token_count, 2 * rows), bf16),
                dma((4,)), dma((2,)), dma((2,)),
                dma((3, groups)), dma((3, groups)), dma((2, groups)), dma((2, groups)),
            ],
            compiler_params=pltpu.CompilerParams(collective_id=0, has_side_effects=True, vmem_limit_bytes=56 * 2**20),
            name="moe_layer",
        )(tokens[0], w_gate.T, expert_ids[0].T, keep_second, w_in, w_out)
        out = pl.pallas_call(
            finish_kernel,
            out_shape=jax.ShapeDtypeStruct((token_count, dim), bf16),
            in_specs=[pl.BlockSpec(memory_space=vmem)] * 3,
            out_specs=pl.BlockSpec(memory_space=pl.ANY),
            scratch_shapes=[vmem((token_count, dim), bf16), dma((8,))],
            compiler_params=pltpu.CompilerParams(vmem_limit_bytes=8 * 2**20),
            name="moe_finish",
        )(acc, cw_end, y_end)
        return out[None]

    group_spec = P(("dp", "ep"))
    return jax.shard_map(local_layer, mesh=mesh, in_specs=(group_spec, P(), group_spec, group_spec, P("ep"), P("ep")), out_specs=group_spec, check_vma=False)
```

```python
import functools

import jax
import jax.numpy as jnp
from jax import lax
from jax.experimental import pallas as pl
from jax.experimental.pallas import tpu as pltpu
from jax.sharding import PartitionSpec as P

MESH = pl.DeviceIdType.MESH
ORDER = (0, 1, 6, 7, 2, 4, 3, 5)
SENDS = (2, 3, 4, 5, 6, 7, 1)
X_PIECES = ((0, 1), (1, 1), (2, 2))
Y_PIECES = ((0, 2), (2, 2))


def peer_of(me, k):
    core, x, y = me % 2, (me // 2) % 2, me // 4
    core_bit, x_bit, y_bit = k % 2, (k // 2) % 2, k // 4
    core = 1 - core if core_bit else core
    x = 1 - x if x_bit else x
    y = 1 - y if y_bit else y
    return (y * 2 + x) * 2 + core


def layer_kernel(
    cap, tok_hbm, wg_hbm, ids_hbm, keep_hbm, win_hbm, wout_hbm, acc, cw_end, y_end,
    tok, wg, ids, keep, slot_of, gates, cols, dmat, xs, xr, ys, yr, hid, wi, wo, cw,
    in_sem, wi_sem, wo_sem, xs_sem, xr_sem, ys_sem, yr_sem,
):
    me = lax.axis_index("ep")
    experts_here = win_hbm.shape[0]
    tokens, dim = tok.shape
    experts = wg.shape[0]
    hidden = hid.shape[1]
    groups = experts // experts_here
    rows = groups * cap
    f32, bf16 = jnp.float32, jnp.bfloat16

    parts = (pl.ds(0, dim // 2), pl.ds(dim // 2, dim // 2))
    small = [
        pltpu.make_async_copy(ids_hbm, ids, in_sem.at[0]),
        pltpu.make_async_copy(keep_hbm, keep, in_sem.at[1]),
    ] + [
        pltpu.make_async_copy(tok_hbm.at[:, part], tok.at[:, part], in_sem.at[2 + i]) for i, part in enumerate(parts)
    ] + [pltpu.make_async_copy(wg_hbm, wg, in_sem.at[4])]
    for copy in small:
        copy.start()

    barrier = pltpu.get_barrier_semaphore()
    for k in range(1, 8):
        pl.semaphore_signal(barrier, inc=1, device_id={"ep": peer_of(me, k)}, device_id_type=MESH)

    def wi_copy(e):
        return pltpu.make_async_copy(win_hbm.at[e], wi.at[e % 2], wi_sem.at[e % 2])

    def wo_copy(e):
        return pltpu.make_async_copy(wout_hbm.at[e], wo.at[e % 2], wo_sem.at[e % 2])

    blk = 256
    r_io = lax.broadcasted_iota(jnp.int32, (blk, blk), 0)
    c_io = lax.broadcasted_iota(jnp.int32, (blk, blk), 1)
    before = jnp.where(r_io < c_io, 1.0, 0.0).astype(bf16)
    ones = jnp.ones((blk, blk), bf16)
    expert_row = lax.broadcasted_iota(jnp.int32, (experts, tokens), 0)
    small[0].wait()
    small[1].wait()
    hot1 = (expert_row == ids[0:1, :]).astype(f32)
    hot2 = ((expert_row == ids[1:2, :]) & (keep[0:1, :] > 0)).astype(f32)
    hot = jnp.concatenate([hot1, hot2], axis=0).astype(bf16)
    blocks = range(tokens // blk)
    stack = jnp.concatenate([hot[:, b * blk:(b + 1) * blk] for b in blocks], axis=0)
    within = jnp.dot(stack, before, preferred_element_type=f32)
    counts = jnp.dot(stack, ones, preferred_element_type=f32)
    both = 2 * experts
    first_total = sum(counts[b * both:b * both + experts] for b in blocks)
    seen = jnp.zeros((both, blk), f32)
    for b in blocks:
        at = slice(b * blk, (b + 1) * blk)
        earlier = within[b * both:(b + 1) * both] + seen
        seen = seen + counts[b * both:(b + 1) * both]
        second = jnp.where(hot2[:, at] > 0, earlier[experts:] + first_total, -1.0)
        slot_of[:, at] = jnp.where(hot1[:, at] > 0, earlier[:experts], second)

    def send(src, dst, send_sem, recv_sem, pieces, i, p):
        at = pl.ds(*pieces[i])
        return pltpu.make_async_remote_copy(
            src_ref=src.at[p, at], dst_ref=y_end.at[p - 6] if dst is yr and i == 1 and p >= 6 else dst.at[p, at],
            send_sem=send_sem.at[i, p], recv_sem=recv_sem.at[i, p],
            device_id={"ep": peer_of(me, ORDER[p])}, device_id_type=MESH,
        )

    x_send = functools.partial(send, xs, xr, xs_sem, xr_sem, X_PIECES)
    y_send = functools.partial(send, ys, yr, ys_sem, yr_sem, Y_PIECES)

    def first_slot(e, p):
        return peer_of(me, ORDER[p]) * (experts_here * cap) + e * cap

    def block_hot(e, p):
        slot = lax.broadcasted_iota(jnp.int32, (cap, tokens), 0).astype(f32)
        taken = slot_of[pl.ds(peer_of(me, ORDER[p]) * experts_here + e, 1), :]
        return jnp.where(slot == taken, 1.0, 0.0).astype(bf16)

    for half in ((1, 2), (3, 0)):
        places = [2 * q + side for q in half for side in (0, 1)]
        for i, p in enumerate(places):
            dmat[i * cap:(i + 1) * cap, :] = block_hot(0, p)
        for n, part in enumerate(parts):
            if half[0] == 1:
                small[2 + n].wait()
            got = jnp.dot(dmat[0:4 * cap, :], tok[:, part], preferred_element_type=f32).astype(bf16)
            for i, p in enumerate(places):
                (xs if p else xr)[p, 0, :, part] = got[i * cap:(i + 1) * cap]
        if half[0] == 1:
            pl.semaphore_wait(barrier, 7)
        for p in places:
            if p:
                x_send(0, p).start()
    for e in range(2):
        wi_copy(e).start()
        wo_copy(e).start()

    def dispatch(e, _):
        for p in range(groups):
            dmat[p * cap:(p + 1) * cap, :] = block_hot(e, p)

        def columns(n, _):
            at = pl.ds(pl.multiple_of(n * blk, blk), blk)
            got = jnp.dot(dmat[...], tok[:, at], preferred_element_type=f32).astype(bf16)
            xs[:, e, :, at] = got.reshape(groups, cap, blk)
            return 0

        lax.fori_loop(0, dim // blk, columns, 0)
        for i, (start, count) in enumerate(X_PIECES[1:], 1):
            @pl.when(e == start + count - 1)
            def _():
                for p in SENDS:
                    x_send(i, p).start()
        xr[0, e] = xs[0, e]
        return 0

    lax.fori_loop(1, experts_here, dispatch, 0)

    small[4].wait()
    logits = lax.dot_general(wg[...], tok[...], (((1,), (1,)), ((), ())), preferred_element_type=f32)
    top = jnp.max(logits, axis=0, keepdims=True)
    expd = jnp.exp(logits - top)
    probs = expd / jnp.sum(expd, axis=0, keepdims=True)
    id1, id2, kept2 = ids[0:1, :], ids[1:2, :], keep[0:1, :] > 0
    is1, is2 = expert_row == id1, (expert_row == id2) & kept2

    def pick(mask, value):
        return jnp.sum(jnp.where(mask, value, 0.0), axis=0, keepdims=True)

    gate1, gate2 = pick(is1, probs), pick(is2, probs)
    slot1, slot2 = pick(is1, slot_of[...]), pick(is2, slot_of[...])
    total = gate1 + gate2
    gates[0:1, :] = jnp.where(slot1 < cap, id1.astype(f32) * cap + slot1, -1.0)
    gates[1:2, :] = jnp.where((slot2 < cap) & kept2, id2.astype(f32) * cap + slot2, -1.0)
    gates[2:3, :] = gate1 / total
    gates[3:4, :] = gate2 / total
    gates[4:, :] = jnp.zeros((gates.shape[0] - 4, tokens), f32)
    cols[...] = gates[...].T

    def weights(i, _):
        def block(t, _):
            at = pl.ds(pl.multiple_of(t * blk, blk), blk)
            lane = lax.broadcasted_iota(jnp.int32, (8, 2 * rows), 1)
            slot = lane
            for p in range(groups):
                slot = slot + jnp.where(lane // (2 * cap) == p, first_slot(2 * i, p) - p * 2 * cap, 0)
            slot = slot[0:1, :].astype(f32)
            part = cols[at, :]
            cw[i, at, :] = (
                jnp.where(slot == part[:, 0:1], part[:, 2:3], 0.0) + jnp.where(slot == part[:, 1:2], part[:, 3:4], 0.0)
            ).astype(bf16)
            return 0

        return lax.fori_loop(0, tokens // blk, block, 0)

    lax.fori_loop(0, experts_here // 2, weights, 0)

    def expert(e, _):
        s = e % 2
        for i, (start, _count) in enumerate(X_PIECES):
            @pl.when(e == start)
            def _():
                for p in SENDS:
                    x_send(i, p).wait_recv()

        wi_copy(e).wait()

        def up(j, _):
            at = pl.ds(pl.multiple_of(j * blk, blk), blk)
            pre = jnp.dot(xr[:, e].reshape(rows, dim), wi[s, :, at], preferred_element_type=f32)
            hid[:, at] = jnp.maximum(pre, 0.0).astype(bf16)
            return 0

        lax.fori_loop(0, hidden // blk, up, 0)

        @pl.when(e + 2 < experts_here)
        def _():
            wi_copy(e + 2).start()

        wo_copy(e).wait()

        def down(n, _):
            at = pl.ds(pl.multiple_of(n * blk, blk), blk)
            got = jnp.dot(hid[...], wo[s, :, at], preferred_element_type=f32).astype(bf16)
            ys[:, e, :, at] = got.reshape(groups, cap, blk)
            return 0

        lax.fori_loop(0, dim // blk, down, 0)

        @pl.when(e + 2 < experts_here)
        def _():
            wo_copy(e + 2).start()

        for i, (start, count) in enumerate(Y_PIECES):
            @pl.when(e == start + count - 1)
            def _():
                for p in SENDS:
                    y_send(i, p).start()
        yr[0, e] = ys[0, e]
        return 0

    lax.fori_loop(0, experts_here, expert, 0)

    for p in SENDS:
        y_send(0, p).wait_recv()

    def columns(n, _):
        at = pl.ds(pl.multiple_of(n * blk, blk), blk)
        acc[:, at] = jnp.dot(cw[0], yr[:, 0:2, :, at].reshape(2 * rows, blk), preferred_element_type=f32)
        return 0

    lax.fori_loop(0, dim // blk, columns, 0)
    for q in range(groups // 2 - 1):
        for p in (2 * q, 2 * q + 1):
            if p:
                y_send(1, p).wait_recv()

        def pair_columns(n, _):
            at = pl.ds(pl.multiple_of(n * blk, blk), blk)
            back = yr[2 * q:2 * q + 2, 2:4, :, at].reshape(4 * cap, blk)
            acc[:, at] += jnp.dot(cw[1, :, q * 4 * cap:(q + 1) * 4 * cap], back, preferred_element_type=f32)
            return 0

        lax.fori_loop(0, dim // blk, pair_columns, 0)
    cw_end[...] = cw[1, :, 2 * rows - 4 * cap:]
    for i in range(len(X_PIECES)):
        for p in SENDS:
            x_send(i, p).wait_send()
    for p in SENDS:
        y_send(0, p).wait_send()
    for p in (groups - 2, groups - 1):
        y_send(1, p).wait_recv()
    for p in SENDS:
        y_send(1, p).wait_send()


def finish_kernel(acc, cw, y, out, buf, sem):
    blk = buf.shape[0] // 8
    copies = []
    for t in range(8):
        at = pl.ds(t * blk, blk)
        buf[at, :] = (acc[at, :] + jnp.dot(cw[at, :], y[...].reshape(cw.shape[1], acc.shape[1]), preferred_element_type=jnp.float32)).astype(out.dtype)
        copies.append(pltpu.make_async_copy(buf.at[at], out.at[at], sem.at[t]))
        copies[-1].start()
    for copy in copies:
        copy.wait()


def solution(mesh):
    def local_layer(tokens, w_gate, expert_ids, keep_second, w_in, w_out):
        _, token_count, dim = tokens.shape
        experts = w_gate.shape[1]
        here, _, hidden = w_in.shape
        cap = 2 * token_count // experts
        groups = experts // here
        rows = groups * cap
        f32, bf16 = jnp.float32, jnp.bfloat16
        vmem, dma = pltpu.VMEM, pltpu.SemaphoreType.DMA
        acc, cw_end, y_end = pl.pallas_call(
            functools.partial(layer_kernel, cap),
            out_shape=(vmem((token_count, dim), f32), vmem((token_count, 4 * cap), bf16), vmem((2, 2, cap, dim), bf16)),
            in_specs=[pl.BlockSpec(memory_space=pl.ANY)] * 6,
            out_specs=[pl.BlockSpec(memory_space=vmem)] * 3,
            scratch_shapes=[
                vmem((token_count, dim), bf16),
                vmem((experts, dim), bf16),
                vmem((2, token_count), jnp.int32),
                vmem((1, token_count), jnp.int32),
                vmem((experts, token_count), f32),
                vmem((128, token_count), f32),
                vmem((token_count, 128), f32),
                vmem((rows, token_count), bf16),
                vmem((groups, here, cap, dim), bf16),
                vmem((groups, here, cap, dim), bf16),
                vmem((groups, here, cap, dim), bf16),
                vmem((groups, here, cap, dim), bf16),
                vmem((rows, hidden), bf16),
                vmem((2, dim, hidden), bf16),
                vmem((2, hidden, dim), bf16),
                vmem((here // 2, token_count, 2 * rows), bf16),
                dma((5,)), dma((2,)), dma((2,)),
                dma((3, groups)), dma((3, groups)), dma((2, groups)), dma((2, groups)),
            ],
            compiler_params=pltpu.CompilerParams(collective_id=0, has_side_effects=True, vmem_limit_bytes=56 * 2**20),
            name="moe_layer",
        )(tokens[0], w_gate.T, expert_ids[0].T, keep_second, w_in, w_out)
        out = pl.pallas_call(
            finish_kernel,
            out_shape=jax.ShapeDtypeStruct((token_count, dim), bf16),
            in_specs=[pl.BlockSpec(memory_space=vmem)] * 3,
            out_specs=pl.BlockSpec(memory_space=pl.ANY),
            scratch_shapes=[vmem((token_count, dim), bf16), dma((8,))],
            compiler_params=pltpu.CompilerParams(vmem_limit_bytes=8 * 2**20),
            name="moe_finish",
        )(acc, cw_end, y_end)
        return out[None]

    group_spec = P(("dp", "ep"))
    return jax.shard_map(local_layer, mesh=mesh, in_specs=(group_spec, P(), group_spec, group_spec, P("ep"), P("ep")), out_specs=group_spec, check_vma=False)
```

```python
import functools

import jax
import jax.numpy as jnp
from jax import lax
from jax.experimental import pallas as pl
from jax.experimental.pallas import tpu as pltpu
from jax.sharding import PartitionSpec as P

MESH = pl.DeviceIdType.MESH
ORDER = (0, 1, 6, 7, 2, 4, 3, 5)
SENDS = (2, 3, 4, 5, 6, 7, 1)
X_PIECES = ((0, 1), (1, 1), (2, 2))
Y_PIECES = ((0, 2), (2, 2))


def peer_of(me, k):
    core, x, y = me % 2, (me // 2) % 2, me // 4
    core_bit, x_bit, y_bit = k % 2, (k // 2) % 2, k // 4
    core = 1 - core if core_bit else core
    x = 1 - x if x_bit else x
    y = 1 - y if y_bit else y
    return (y * 2 + x) * 2 + core


def layer_kernel(
    cap, tok_hbm, wg_hbm, ids_hbm, keep_hbm, win_hbm, wout_hbm, acc, cw_end, y_end,
    tok, wg, ids, keep, slot_of, gates, cols, dmat, xs, xr, ys, yr, hid, wi, wo, cw,
    in_sem, wi_sem, wo_sem, xs_sem, xr_sem, ys_sem, yr_sem,
):
    me = lax.axis_index("ep")
    experts_here = win_hbm.shape[0]
    tokens, dim = tok.shape
    experts = wg.shape[0]
    hidden = hid.shape[1]
    groups = experts // experts_here
    rows = groups * cap
    f32, bf16 = jnp.float32, jnp.bfloat16

    parts = (pl.ds(0, dim // 2), pl.ds(dim // 2, dim // 2))
    small = [
        pltpu.make_async_copy(ids_hbm, ids, in_sem.at[0]),
        pltpu.make_async_copy(keep_hbm, keep, in_sem.at[1]),
    ] + [
        pltpu.make_async_copy(tok_hbm.at[:, part], tok.at[:, part], in_sem.at[2 + i]) for i, part in enumerate(parts)
    ] + [pltpu.make_async_copy(wg_hbm, wg, in_sem.at[4])]
    for copy in small:
        copy.start()

    barrier = pltpu.get_barrier_semaphore()
    for k in range(1, 8):
        pl.semaphore_signal(barrier, inc=1, device_id={"ep": peer_of(me, k)}, device_id_type=MESH)

    def wi_copy(e):
        return pltpu.make_async_copy(win_hbm.at[e], wi.at[e % 2], wi_sem.at[e % 2])

    def wo_copy(e):
        return pltpu.make_async_copy(wout_hbm.at[e], wo.at[e % 2], wo_sem.at[e % 2])

    blk = 256
    r_io = lax.broadcasted_iota(jnp.int32, (blk, blk), 0)
    c_io = lax.broadcasted_iota(jnp.int32, (blk, blk), 1)
    before = jnp.where(r_io < c_io, 1.0, 0.0).astype(bf16)
    ones = jnp.ones((blk, blk), bf16)
    expert_row = lax.broadcasted_iota(jnp.int32, (experts, tokens), 0)
    small[0].wait()
    small[1].wait()
    hot1 = (expert_row == ids[0:1, :]).astype(f32)
    hot2 = ((expert_row == ids[1:2, :]) & (keep[0:1, :] > 0)).astype(f32)
    hot = jnp.concatenate([hot1, hot2], axis=0).astype(bf16)
    blocks = range(tokens // blk)
    stack = jnp.concatenate([hot[:, b * blk:(b + 1) * blk] for b in blocks], axis=0)
    within = jnp.dot(stack, before, preferred_element_type=f32)
    counts = jnp.dot(stack, ones, preferred_element_type=f32)
    both = 2 * experts
    first_total = sum(counts[b * both:b * both + experts] for b in blocks)
    seen = jnp.zeros((both, blk), f32)
    for b in blocks:
        at = slice(b * blk, (b + 1) * blk)
        earlier = within[b * both:(b + 1) * both] + seen
        seen = seen + counts[b * both:(b + 1) * both]
        second = jnp.where(hot2[:, at] > 0, earlier[experts:] + first_total, -1.0)
        slot_of[:, at] = jnp.where(hot1[:, at] > 0, earlier[:experts], second)

    def copy_to(p, src, dst, send_sem, recv_sem):
        return pltpu.make_async_remote_copy(
            src_ref=src, dst_ref=dst, send_sem=send_sem, recv_sem=recv_sem,
            device_id={"ep": peer_of(me, ORDER[p])}, device_id_type=MESH,
        )

    def x_send(i, p):
        at = pl.ds(*X_PIECES[i])
        return copy_to(p, xs.at[p, at], xr.at[p, at], xs_sem.at[0], xr_sem.at[i])

    def x_wait(i):
        at, places = pl.ds(*X_PIECES[i]), pl.ds(1, groups - 1)
        copy_to(1, xs.at[places, at], xr.at[places, at], xs_sem.at[0], xr_sem.at[i]).wait_recv()

    def y_send(i, p):
        at = pl.ds(*Y_PIECES[i])
        to = y_end.at[p - 6] if i == 1 and p >= 6 else yr.at[p, at]
        return copy_to(p, ys.at[p, at], to, ys_sem.at[0], yr_sem.at[1 + p // 2 if i else 0])

    def y_wait(i, first, count):
        at, places = pl.ds(*Y_PIECES[i]), pl.ds(first, count)
        to = y_end if i == 1 and first >= 6 else yr.at[places, at]
        copy_to(1, ys.at[places, at], to, ys_sem.at[0], yr_sem.at[1 + first // 2 if i else 0]).wait_recv()

    def first_slot(e, p):
        return peer_of(me, ORDER[p]) * (experts_here * cap) + e * cap

    def block_hot(e, p):
        slot = lax.broadcasted_iota(jnp.int32, (cap, tokens), 0).astype(f32)
        taken = slot_of[pl.ds(peer_of(me, ORDER[p]) * experts_here + e, 1), :]
        return jnp.where(slot == taken, 1.0, 0.0).astype(bf16)

    for half in ((1, 2), (3, 0)):
        places = [2 * q + side for q in half for side in (0, 1)]
        for i, p in enumerate(places):
            dmat[i * cap:(i + 1) * cap, :] = block_hot(0, p)
        for n, part in enumerate(parts):
            if half[0] == 1:
                small[2 + n].wait()
            got = jnp.dot(dmat[0:4 * cap, :], tok[:, part], preferred_element_type=f32).astype(bf16)
            for i, p in enumerate(places):
                (xs if p else xr)[p, 0, :, part] = got[i * cap:(i + 1) * cap]
        if half[0] == 1:
            pl.semaphore_wait(barrier, 7)
        for p in places:
            if p:
                x_send(0, p).start()
    for e in range(2):
        wi_copy(e).start()
        wo_copy(e).start()

    def dispatch(e, _):
        for p in range(groups):
            dmat[p * cap:(p + 1) * cap, :] = block_hot(e, p)

        def columns(n, _):
            at = pl.ds(pl.multiple_of(n * blk, blk), blk)
            got = jnp.dot(dmat[...], tok[:, at], preferred_element_type=f32).astype(bf16)
            xs[:, e, :, at] = got.reshape(groups, cap, blk)
            return 0

        lax.fori_loop(0, dim // blk, columns, 0)
        for i, (start, count) in enumerate(X_PIECES[1:], 1):
            @pl.when(e == start + count - 1)
            def _():
                for p in SENDS:
                    x_send(i, p).start()
        xr[0, e] = xs[0, e]
        return 0

    lax.fori_loop(1, experts_here, dispatch, 0)

    small[4].wait()
    logits = lax.dot_general(wg[...], tok[...], (((1,), (1,)), ((), ())), preferred_element_type=f32)
    top = jnp.max(logits, axis=0, keepdims=True)
    expd = jnp.exp(logits - top)
    probs = expd / jnp.sum(expd, axis=0, keepdims=True)
    id1, id2, kept2 = ids[0:1, :], ids[1:2, :], keep[0:1, :] > 0
    is1, is2 = expert_row == id1, (expert_row == id2) & kept2

    def pick(mask, value):
        return jnp.sum(jnp.where(mask, value, 0.0), axis=0, keepdims=True)

    gate1, gate2 = pick(is1, probs), pick(is2, probs)
    slot1, slot2 = pick(is1, slot_of[...]), pick(is2, slot_of[...])
    total = gate1 + gate2
    gates[0:1, :] = jnp.where(slot1 < cap, id1.astype(f32) * cap + slot1, -1.0)
    gates[1:2, :] = jnp.where((slot2 < cap) & kept2, id2.astype(f32) * cap + slot2, -1.0)
    gates[2:3, :] = gate1 / total
    gates[3:4, :] = gate2 / total
    gates[4:, :] = jnp.zeros((gates.shape[0] - 4, tokens), f32)
    cols[...] = gates[...].T

    def weights(i, _):
        def block(t, _):
            at = pl.ds(pl.multiple_of(t * blk, blk), blk)
            lane = lax.broadcasted_iota(jnp.int32, (8, 2 * rows), 1)
            slot = lane
            for p in range(groups):
                slot = slot + jnp.where(lane // (2 * cap) == p, first_slot(2 * i, p) - p * 2 * cap, 0)
            slot = slot[0:1, :].astype(f32)
            part = cols[at, :]
            cw[i, at, :] = (
                jnp.where(slot == part[:, 0:1], part[:, 2:3], 0.0) + jnp.where(slot == part[:, 1:2], part[:, 3:4], 0.0)
            ).astype(bf16)
            return 0

        return lax.fori_loop(0, tokens // blk, block, 0)

    lax.fori_loop(0, experts_here // 2, weights, 0)

    def expert(e, _):
        s = e % 2
        for i, (start, _count) in enumerate(X_PIECES):
            @pl.when(e == start)
            def _():
                x_wait(i)

        wi_copy(e).wait()

        def up(j, _):
            at = pl.ds(pl.multiple_of(j * blk, blk), blk)
            pre = jnp.dot(xr[:, e].reshape(rows, dim), wi[s, :, at], preferred_element_type=f32)
            hid[:, at] = jnp.maximum(pre, 0.0).astype(bf16)
            return 0

        lax.fori_loop(0, hidden // blk, up, 0)

        @pl.when(e + 2 < experts_here)
        def _():
            wi_copy(e + 2).start()

        wo_copy(e).wait()

        def down(n, _):
            at = pl.ds(pl.multiple_of(n * blk, blk), blk)
            got = jnp.dot(hid[...], wo[s, :, at], preferred_element_type=f32).astype(bf16)
            ys[:, e, :, at] = got.reshape(groups, cap, blk)
            return 0

        lax.fori_loop(0, dim // blk, down, 0)

        @pl.when(e + 2 < experts_here)
        def _():
            wo_copy(e + 2).start()

        for i, (start, count) in enumerate(Y_PIECES):
            @pl.when(e == start + count - 1)
            def _():
                for p in SENDS:
                    y_send(i, p).start()
        yr[0, e] = ys[0, e]
        return 0

    lax.fori_loop(0, experts_here, expert, 0)

    y_wait(0, 1, groups - 1)

    def columns(n, _):
        at = pl.ds(pl.multiple_of(n * blk, blk), blk)
        acc[:, at] = jnp.dot(cw[0], yr[:, 0:2, :, at].reshape(2 * rows, blk), preferred_element_type=f32)
        return 0

    lax.fori_loop(0, dim // blk, columns, 0)
    for q in range(groups // 2 - 1):
        y_wait(1, max(2 * q, 1), 2 if q else 1)

        def pair_columns(n, _):
            at = pl.ds(pl.multiple_of(n * blk, blk), blk)
            back = yr[2 * q:2 * q + 2, 2:4, :, at].reshape(4 * cap, blk)
            acc[:, at] += jnp.dot(cw[1, :, q * 4 * cap:(q + 1) * 4 * cap], back, preferred_element_type=f32)
            return 0

        lax.fori_loop(0, dim // blk, pair_columns, 0)
    cw_end[...] = cw[1, :, 2 * rows - 4 * cap:]
    sent = pl.ds(1, groups - 1)
    copy_to(1, xs.at[sent], xr.at[sent], xs_sem.at[0], xr_sem.at[0]).wait_send()
    y_wait(1, groups - 2, 2)
    copy_to(1, ys.at[sent], yr.at[sent], ys_sem.at[0], yr_sem.at[0]).wait_send()


def finish_kernel(acc, cw, y, out, buf, sem):
    blk = buf.shape[0] // 8
    for t in range(8):
        at = pl.ds(t * blk, blk)
        buf[at, :] = (acc[at, :] + jnp.dot(cw[at, :], y[...].reshape(cw.shape[1], acc.shape[1]), preferred_element_type=jnp.float32)).astype(out.dtype)
        pltpu.make_async_copy(buf.at[at], out.at[at], sem.at[0]).start()
    pltpu.make_async_copy(buf, out, sem.at[0]).wait()


def solution(mesh):
    def local_layer(tokens, w_gate, expert_ids, keep_second, w_in, w_out):
        _, token_count, dim = tokens.shape
        experts = w_gate.shape[1]
        here, _, hidden = w_in.shape
        cap = 2 * token_count // experts
        groups = experts // here
        rows = groups * cap
        f32, bf16 = jnp.float32, jnp.bfloat16
        vmem, dma = pltpu.VMEM, pltpu.SemaphoreType.DMA
        acc, cw_end, y_end = pl.pallas_call(
            functools.partial(layer_kernel, cap),
            out_shape=(vmem((token_count, dim), f32), vmem((token_count, 4 * cap), bf16), vmem((2, 2, cap, dim), bf16)),
            in_specs=[pl.BlockSpec(memory_space=pl.ANY)] * 6,
            out_specs=[pl.BlockSpec(memory_space=vmem)] * 3,
            scratch_shapes=[
                vmem((token_count, dim), bf16),
                vmem((experts, dim), bf16),
                vmem((2, token_count), jnp.int32),
                vmem((1, token_count), jnp.int32),
                vmem((experts, token_count), f32),
                vmem((128, token_count), f32),
                vmem((token_count, 128), f32),
                vmem((rows, token_count), bf16),
                vmem((groups, here, cap, dim), bf16),
                vmem((groups, here, cap, dim), bf16),
                vmem((groups, here, cap, dim), bf16),
                vmem((groups, here, cap, dim), bf16),
                vmem((rows, hidden), bf16),
                vmem((2, dim, hidden), bf16),
                vmem((2, hidden, dim), bf16),
                vmem((here // 2, token_count, 2 * rows), bf16),
                dma((5,)), dma((2,)), dma((2,)),
                dma((1,)), dma((3,)), dma((1,)), dma((5,)),
            ],
            compiler_params=pltpu.CompilerParams(collective_id=0, has_side_effects=True, vmem_limit_bytes=56 * 2**20),
            name="moe_layer",
        )(tokens[0], w_gate.T, expert_ids[0].T, keep_second, w_in, w_out)
        out = pl.pallas_call(
            finish_kernel,
            out_shape=jax.ShapeDtypeStruct((token_count, dim), bf16),
            in_specs=[pl.BlockSpec(memory_space=vmem)] * 3,
            out_specs=pl.BlockSpec(memory_space=pl.ANY),
            scratch_shapes=[vmem((token_count, dim), bf16), dma((1,))],
            compiler_params=pltpu.CompilerParams(vmem_limit_bytes=8 * 2**20),
            name="moe_finish",
        )(acc, cw_end, y_end)
        return out[None]

    group_spec = P(("dp", "ep"))
    return jax.shard_map(local_layer, mesh=mesh, in_specs=(group_spec, P(), group_spec, group_spec, P("ep"), P("ep")), out_specs=group_spec, check_vma=False)
```

```python
import functools

import jax
import jax.numpy as jnp
from jax import lax
from jax.experimental import pallas as pl
from jax.experimental.pallas import tpu as pltpu
from jax.sharding import PartitionSpec as P

MESH = pl.DeviceIdType.MESH
ORDER = (0, 1, 6, 7, 2, 4, 3, 5)
SENDS = (2, 3, 4, 5, 6, 7, 1)
X_PIECES = ((0, 1), (1, 1), (2, 2))
Y_PIECES = ((0, 2), (2, 1), (2, 2))
NEAR, FAR = (4, 5, 6, 7), (2, 3, 1)
HELD = 16
CW_BLOCKS = (
    tuple((p, e) for p in range(8) for e in (0, 1)),
    tuple((p, e) for p in range(4) for e in (2, 3)) + tuple((p, e) for e in (2, 3) for p in NEAR),
)


def peer_of(me, k):
    core, x, y = me % 2, (me // 2) % 2, me // 4
    core_bit, x_bit, y_bit = k % 2, (k // 2) % 2, k // 4
    core = 1 - core if core_bit else core
    x = 1 - x if x_bit else x
    y = 1 - y if y_bit else y
    return (y * 2 + x) * 2 + core


def layer_kernel(
    cap, tok_hbm, wg_hbm, ids_hbm, keep_hbm, win_hbm, wout_hbm, acc, cw_end, y_end,
    tok, wg, ids, keep, slot_of, gates, cols, slots, dmat, xs, xr, ys, yr, hid, wi, wo, cw,
    in_sem, wi_sem, wo_sem, xs_sem, xr_sem, ys_sem, yr_sem,
):
    me = lax.axis_index("ep")
    experts_here = win_hbm.shape[0]
    tokens, dim = tok.shape
    experts = wg.shape[0]
    hidden = hid.shape[1]
    groups = experts // experts_here
    rows = groups * cap
    f32, bf16 = jnp.float32, jnp.bfloat16

    parts = (pl.ds(0, dim // 2), pl.ds(dim // 2, dim // 2))
    small = [
        pltpu.make_async_copy(ids_hbm, ids, in_sem.at[0]),
        pltpu.make_async_copy(keep_hbm, keep, in_sem.at[1]),
    ] + [
        pltpu.make_async_copy(tok_hbm.at[:, part], tok.at[:, part], in_sem.at[2 + i]) for i, part in enumerate(parts)
    ] + [pltpu.make_async_copy(wg_hbm, wg, in_sem.at[4])]
    for copy in small:
        copy.start()

    barrier = pltpu.get_barrier_semaphore()
    for k in range(1, 8):
        pl.semaphore_signal(barrier, inc=1, device_id={"ep": peer_of(me, k)}, device_id_type=MESH)

    def wi_copy(e):
        return pltpu.make_async_copy(win_hbm.at[e], wi.at[e % 2], wi_sem.at[e % 2])

    def wo_copy(e):
        return pltpu.make_async_copy(wout_hbm.at[e], wo.at[e % 2], wo_sem.at[e % 2])

    blk = 256
    r_io = lax.broadcasted_iota(jnp.int32, (blk, blk), 0)
    c_io = lax.broadcasted_iota(jnp.int32, (blk, blk), 1)
    before = jnp.where(r_io < c_io, 1.0, 0.0).astype(bf16)
    ones = jnp.ones((blk, blk), bf16)
    expert_row = lax.broadcasted_iota(jnp.int32, (experts, tokens), 0)
    small[0].wait()
    small[1].wait()
    hot1 = (expert_row == ids[0:1, :]).astype(f32)
    hot2 = ((expert_row == ids[1:2, :]) & (keep[0:1, :] > 0)).astype(f32)
    hot = jnp.concatenate([hot1, hot2], axis=0).astype(bf16)
    blocks = range(tokens // blk)
    stack = jnp.concatenate([hot[:, b * blk:(b + 1) * blk] for b in blocks], axis=0)
    within = jnp.dot(stack, before, preferred_element_type=f32)
    counts = jnp.dot(stack, ones, preferred_element_type=f32)
    both = 2 * experts
    first_total = sum(counts[b * both:b * both + experts] for b in blocks)
    seen = jnp.zeros((both, blk), f32)
    for b in blocks:
        at = slice(b * blk, (b + 1) * blk)
        earlier = within[b * both:(b + 1) * both] + seen
        seen = seen + counts[b * both:(b + 1) * both]
        second = jnp.where(hot2[:, at] > 0, earlier[experts:] + first_total, -1.0)
        slot_of[:, at] = jnp.where(hot1[:, at] > 0, earlier[:experts], second)

    def copy_to(p, src, dst, send_sem, recv_sem):
        return pltpu.make_async_remote_copy(
            src_ref=src, dst_ref=dst, send_sem=send_sem, recv_sem=recv_sem,
            device_id={"ep": peer_of(me, ORDER[p])}, device_id_type=MESH,
        )

    def x_send(i, p):
        at = pl.ds(*X_PIECES[i])
        return copy_to(p, xs.at[p, at], xr.at[p, at], xs_sem.at[0], xr_sem.at[i])

    def x_wait(i):
        at, places = pl.ds(*X_PIECES[i]), pl.ds(1, groups - 1)
        copy_to(1, xs.at[places, at], xr.at[places, at], xs_sem.at[0], xr_sem.at[i]).wait_recv()

    def y_send(i, p):
        at = pl.ds(*Y_PIECES[i])
        return copy_to(p, ys.at[p, at], yr.at[p, at], ys_sem.at[0], yr_sem.at[(0, 1, 2 + p // 2)[i]])

    def y_wait(i, first, count):
        at, places = pl.ds(*Y_PIECES[i]), pl.ds(first, count)
        copy_to(1, ys.at[places, at], yr.at[places, at], ys_sem.at[0], yr_sem.at[(0, 1, 2 + first // 2)[i]]).wait_recv()

    def end_send(p, first, count):
        at = pl.ds(first, count)
        return copy_to(p, ys.at[p, experts_here - 1, at], y_end.at[p - 4, at], ys_sem.at[0], yr_sem.at[4])

    def first_slot(e, p):
        return peer_of(me, ORDER[p]) * (experts_here * cap) + e * cap

    def block_hot(e, p):
        slot = lax.broadcasted_iota(jnp.int32, (cap, tokens), 0).astype(f32)
        taken = slot_of[pl.ds(peer_of(me, ORDER[p]) * experts_here + e, 1), :]
        return jnp.where(slot == taken, 1.0, 0.0).astype(bf16)

    for half in ((1, 2), (3, 0)):
        places = [2 * q + side for q in half for side in (0, 1)]
        for i, p in enumerate(places):
            dmat[i * cap:(i + 1) * cap, :] = block_hot(0, p)
        for n, part in enumerate(parts):
            if half[0] == 1:
                small[2 + n].wait()
            got = jnp.dot(dmat[0:4 * cap, :], tok[:, part], preferred_element_type=f32).astype(bf16)
            for i, p in enumerate(places):
                (xs if p else xr)[p, 0, :, part] = got[i * cap:(i + 1) * cap]
        if half[0] == 1:
            pl.semaphore_wait(barrier, 7)
        for p in places:
            if p:
                x_send(0, p).start()
    for e in range(2):
        wi_copy(e).start()
        wo_copy(e).start()

    def dispatch(e, _):
        for p in range(groups):
            dmat[p * cap:(p + 1) * cap, :] = block_hot(e, p)

        def columns(n, _):
            at = pl.ds(pl.multiple_of(n * blk, blk), blk)
            got = jnp.dot(dmat[...], tok[:, at], preferred_element_type=f32).astype(bf16)
            xs[:, e, :, at] = got.reshape(groups, cap, blk)
            return 0

        lax.fori_loop(0, dim // blk, columns, 0)
        for i, (start, count) in enumerate(X_PIECES[1:], 1):
            @pl.when(e == start + count - 1)
            def _():
                for p in SENDS:
                    x_send(i, p).start()
        xr[0, e] = xs[0, e]
        return 0

    lax.fori_loop(1, experts_here, dispatch, 0)

    small[4].wait()
    logits = lax.dot_general(wg[...], tok[...], (((1,), (1,)), ((), ())), preferred_element_type=f32)
    top = jnp.max(logits, axis=0, keepdims=True)
    expd = jnp.exp(logits - top)
    probs = expd / jnp.sum(expd, axis=0, keepdims=True)
    id1, id2, kept2 = ids[0:1, :], ids[1:2, :], keep[0:1, :] > 0
    is1, is2 = expert_row == id1, (expert_row == id2) & kept2

    def pick(mask, value):
        return jnp.sum(jnp.where(mask, value, 0.0), axis=0, keepdims=True)

    gate1, gate2 = pick(is1, probs), pick(is2, probs)
    slot1, slot2 = pick(is1, slot_of[...]), pick(is2, slot_of[...])
    total = gate1 + gate2
    gates[0:1, :] = jnp.where(slot1 < cap, id1.astype(f32) * cap + slot1, -1.0)
    gates[1:2, :] = jnp.where((slot2 < cap) & kept2, id2.astype(f32) * cap + slot2, -1.0)
    gates[2:3, :] = gate1 / total
    gates[3:4, :] = gate2 / total
    gates[4:, :] = jnp.zeros((gates.shape[0] - 4, tokens), f32)
    cols[...] = gates[...].T

    for i, order in enumerate(CW_BLOCKS):
        lane = lax.broadcasted_iota(jnp.int32, (8, 2 * rows), 1)
        slot = lane
        for b, (p, e) in enumerate(order):
            slot = slot + jnp.where(lane // cap == b, first_slot(e, p) - b * cap, 0)
        slots[i] = slot.astype(f32)

    def weights(i, _):
        def block(t, _):
            at = pl.ds(pl.multiple_of(t * blk, blk), blk)
            slot = slots[i, 0:1, :]
            part = cols[at, :]
            cw[i, at, :] = (
                jnp.where(slot == part[:, 0:1], part[:, 2:3], 0.0) + jnp.where(slot == part[:, 1:2], part[:, 3:4], 0.0)
            ).astype(bf16)
            return 0

        return lax.fori_loop(0, tokens // blk, block, 0)

    lax.fori_loop(0, experts_here // 2, weights, 0)

    def expert(e, _):
        s = e % 2
        for i, (start, _count) in enumerate(X_PIECES):
            @pl.when(e == start)
            def _():
                x_wait(i)

        wi_copy(e).wait()

        def up(j, _):
            at = pl.ds(pl.multiple_of(j * blk, blk), blk)
            pre = jnp.dot(xr[:, e].reshape(rows, dim), wi[s, :, at], preferred_element_type=f32)
            hid[:, at] = jnp.maximum(pre, 0.0).astype(bf16)
            return 0

        lax.fori_loop(0, hidden // blk, up, 0)

        @pl.when(e + 2 < experts_here)
        def _():
            wi_copy(e + 2).start()

        wo_copy(e).wait()

        def down(n, _):
            at = pl.ds(pl.multiple_of(n * blk, blk), blk)
            got = jnp.dot(hid[...], wo[s, :, at], preferred_element_type=f32).astype(bf16)
            ys[:, e, :, at] = got.reshape(groups, cap, blk)
            return 0

        lax.fori_loop(0, dim // blk, down, 0)

        @pl.when(e + 2 < experts_here)
        def _():
            wo_copy(e + 2).start()

        @pl.when(e == 1)
        def _():
            for p in SENDS:
                y_send(0, p).start()

        @pl.when(e == 2)
        def _():
            for p in NEAR:
                y_send(1, p).start()

        @pl.when(e == 3)
        def _():
            for p in FAR:
                y_send(2, p).start()

        @pl.when((e == 3) & (me % 2 == 0))
        def _():
            for p in NEAR:
                end_send(p, 0, cap).start()

        @pl.when((e == 3) & (me % 2 == 1))
        def _():
            for p, first, count in [(p, 0, cap - HELD) for p in (4, 5)] + [(p, 0, cap) for p in (6, 7)] + [(p, cap - HELD, HELD) for p in (4, 5)]:
                end_send(p, first, count).start()

        yr[0, e] = ys[0, e]
        return 0

    lax.fori_loop(0, experts_here, expert, 0)

    y_wait(0, 1, groups - 1)

    def columns(n, _):
        at = pl.ds(pl.multiple_of(n * blk, blk), blk)
        acc[:, at] = jnp.dot(cw[0], yr[:, 0:2, :, at].reshape(2 * rows, blk), preferred_element_type=f32)
        return 0

    lax.fori_loop(0, dim // blk, columns, 0)
    def add_rows(first, back_of):
        def part(n, _):
            at = pl.ds(pl.multiple_of(n * blk, blk), blk)
            acc[:, at] += jnp.dot(cw[1, :, first:first + 4 * cap], back_of(at).reshape(4 * cap, blk), preferred_element_type=f32)
            return 0

        lax.fori_loop(0, dim // blk, part, 0)

    y_wait(1, 4, 4)
    add_rows(rows, lambda at: yr[4:8, 2, :, at])
    y_wait(2, 1, 1)
    add_rows(0, lambda at: yr[0:2, 2:4, :, at])
    y_wait(2, 2, 2)
    add_rows(4 * cap, lambda at: yr[2:4, 2:4, :, at])
    cw_end[...] = cw[1, :, 2 * rows - 4 * cap:]
    sent = pl.ds(1, groups - 1)
    copy_to(1, xs.at[sent], xr.at[sent], xs_sem.at[0], xr_sem.at[0]).wait_send()
    copy_to(1, ys.at[4:8, 0], y_end, ys_sem.at[0], yr_sem.at[4]).wait_recv()
    copy_to(1, ys.at[sent], yr.at[sent], ys_sem.at[0], yr_sem.at[0]).wait_send()


def finish_kernel(acc, cw, y, out, buf, sem):
    blk = buf.shape[0] // 8
    for t in range(8):
        at = pl.ds(t * blk, blk)
        buf[at, :] = (acc[at, :] + jnp.dot(cw[at, :], y[...].reshape(cw.shape[1], acc.shape[1]), preferred_element_type=jnp.float32)).astype(out.dtype)
        pltpu.make_async_copy(buf.at[at], out.at[at], sem.at[0]).start()
    pltpu.make_async_copy(buf, out, sem.at[0]).wait()


def solution(mesh):
    def local_layer(tokens, w_gate, expert_ids, keep_second, w_in, w_out):
        _, token_count, dim = tokens.shape
        experts = w_gate.shape[1]
        here, _, hidden = w_in.shape
        cap = 2 * token_count // experts
        groups = experts // here
        rows = groups * cap
        f32, bf16 = jnp.float32, jnp.bfloat16
        vmem, dma = pltpu.VMEM, pltpu.SemaphoreType.DMA
        acc, cw_end, y_end = pl.pallas_call(
            functools.partial(layer_kernel, cap),
            out_shape=(vmem((token_count, dim), f32), vmem((token_count, 4 * cap), bf16), vmem((4, cap, dim), bf16)),
            in_specs=[pl.BlockSpec(memory_space=pl.ANY)] * 6,
            out_specs=[pl.BlockSpec(memory_space=vmem)] * 3,
            scratch_shapes=[
                vmem((token_count, dim), bf16),
                vmem((experts, dim), bf16),
                vmem((2, token_count), jnp.int32),
                vmem((1, token_count), jnp.int32),
                vmem((experts, token_count), f32),
                vmem((128, token_count), f32),
                vmem((token_count, 128), f32),
                vmem((2, 8, 2 * rows), f32),
                vmem((rows, token_count), bf16),
                vmem((groups, here, cap, dim), bf16),
                vmem((groups, here, cap, dim), bf16),
                vmem((groups, here, cap, dim), bf16),
                vmem((groups, here, cap, dim), bf16),
                vmem((rows, hidden), bf16),
                vmem((2, dim, hidden), bf16),
                vmem((2, hidden, dim), bf16),
                vmem((here // 2, token_count, 2 * rows), bf16),
                dma((5,)), dma((2,)), dma((2,)),
                dma((1,)), dma((3,)), dma((1,)), dma((5,)),
            ],
            compiler_params=pltpu.CompilerParams(collective_id=0, has_side_effects=True, vmem_limit_bytes=56 * 2**20),
            name="moe_layer",
        )(tokens[0], w_gate.T, expert_ids[0].T, keep_second, w_in, w_out)
        out = pl.pallas_call(
            finish_kernel,
            out_shape=jax.ShapeDtypeStruct((token_count, dim), bf16),
            in_specs=[pl.BlockSpec(memory_space=vmem)] * 3,
            out_specs=pl.BlockSpec(memory_space=pl.ANY),
            scratch_shapes=[vmem((token_count, dim), bf16), dma((1,))],
            compiler_params=pltpu.CompilerParams(vmem_limit_bytes=8 * 2**20),
            name="moe_finish",
        )(acc, cw_end, y_end)
        return out[None]

    group_spec = P(("dp", "ep"))
    return jax.shard_map(local_layer, mesh=mesh, in_specs=(group_spec, P(), group_spec, group_spec, P("ep"), P("ep")), out_specs=group_spec, check_vma=False)
```

```python
import functools

import jax
import jax.numpy as jnp
from jax import lax
from jax.experimental import pallas as pl
from jax.experimental.pallas import tpu as pltpu
from jax.sharding import PartitionSpec as P

MESH = pl.DeviceIdType.MESH
ORDER = (0, 1, 6, 7, 2, 4, 3, 5)
SENDS = (2, 3, 4, 5, 6, 7, 1)
X_PIECES = ((0, 1), (1, 1), (2, 2))
Y_PIECES = ((0, 2), (2, 1), (2, 2))
NEAR, FAR = (4, 5, 6, 7), (2, 3, 1)
HELD = 16
HOP = 16
CW_BLOCKS = (
    tuple((p, e) for p in range(8) for e in (0, 1)),
    tuple((p, e) for p in range(4) for e in (2, 3)) + tuple((p, e) for e in (2, 3) for p in NEAR),
)


def peer_of(me, k):
    core, x, y = me % 2, (me // 2) % 2, me // 4
    core_bit, x_bit, y_bit = k % 2, (k // 2) % 2, k // 4
    core = 1 - core if core_bit else core
    x = 1 - x if x_bit else x
    y = 1 - y if y_bit else y
    return (y * 2 + x) * 2 + core


def layer_kernel(
    cap, tok_hbm, wg_hbm, ids_hbm, keep_hbm, win_hbm, wout_hbm, acc, cw_end, y_end,
    tok, wg, ids, keep, slot_of, gates, cols, slots, hop, dmat, xs, xr, ys, yr, hid, wi, wo, cw,
    in_sem, wi_sem, wo_sem, xs_sem, xr_sem, ys_sem, yr_sem, hop_sem,
):
    me = lax.axis_index("ep")
    experts_here = win_hbm.shape[0]
    tokens, dim = tok.shape
    experts = wg.shape[0]
    hidden = hid.shape[1]
    groups = experts // experts_here
    rows = groups * cap
    f32, bf16 = jnp.float32, jnp.bfloat16

    parts = (pl.ds(0, dim // 2), pl.ds(dim // 2, dim // 2))
    small = [
        pltpu.make_async_copy(ids_hbm, ids, in_sem.at[0]),
        pltpu.make_async_copy(keep_hbm, keep, in_sem.at[1]),
    ] + [
        pltpu.make_async_copy(tok_hbm.at[:, part], tok.at[:, part], in_sem.at[2 + i]) for i, part in enumerate(parts)
    ] + [pltpu.make_async_copy(wg_hbm, wg, in_sem.at[4])]
    for copy in small:
        copy.start()

    barrier = pltpu.get_barrier_semaphore()
    for k in range(1, 8):
        pl.semaphore_signal(barrier, inc=1, device_id={"ep": peer_of(me, k)}, device_id_type=MESH)

    def wi_copy(e):
        return pltpu.make_async_copy(win_hbm.at[e], wi.at[e % 2], wi_sem.at[e % 2])

    def wo_copy(e):
        return pltpu.make_async_copy(wout_hbm.at[e], wo.at[e % 2], wo_sem.at[e % 2])

    blk = 256
    r_io = lax.broadcasted_iota(jnp.int32, (blk, blk), 0)
    c_io = lax.broadcasted_iota(jnp.int32, (blk, blk), 1)
    before = jnp.where(r_io < c_io, 1.0, 0.0).astype(bf16)
    ones = jnp.ones((blk, blk), bf16)
    expert_row = lax.broadcasted_iota(jnp.int32, (experts, tokens), 0)
    small[0].wait()
    small[1].wait()
    hot1 = (expert_row == ids[0:1, :]).astype(f32)
    hot2 = ((expert_row == ids[1:2, :]) & (keep[0:1, :] > 0)).astype(f32)
    hot = jnp.concatenate([hot1, hot2], axis=0).astype(bf16)
    blocks = range(tokens // blk)
    stack = jnp.concatenate([hot[:, b * blk:(b + 1) * blk] for b in blocks], axis=0)
    within = jnp.dot(stack, before, preferred_element_type=f32)
    counts = jnp.dot(stack, ones, preferred_element_type=f32)
    both = 2 * experts
    first_total = sum(counts[b * both:b * both + experts] for b in blocks)
    seen = jnp.zeros((both, blk), f32)
    for b in blocks:
        at = slice(b * blk, (b + 1) * blk)
        earlier = within[b * both:(b + 1) * both] + seen
        seen = seen + counts[b * both:(b + 1) * both]
        second = jnp.where(hot2[:, at] > 0, earlier[experts:] + first_total, -1.0)
        slot_of[:, at] = jnp.where(hot1[:, at] > 0, earlier[:experts], second)

    def copy_to(p, src, dst, send_sem, recv_sem):
        return pltpu.make_async_remote_copy(
            src_ref=src, dst_ref=dst, send_sem=send_sem, recv_sem=recv_sem,
            device_id={"ep": peer_of(me, ORDER[p])}, device_id_type=MESH,
        )

    def x_send(i, p):
        at = pl.ds(*X_PIECES[i])
        return copy_to(p, xs.at[p, at], xr.at[p, at], xs_sem.at[0], xr_sem.at[i])

    def far_send(e, first, count):
        at = pl.ds(first, count)
        return copy_to(2, xs.at[2, e, at], xr.at[2, e, at], xs_sem.at[0], xr_sem.at[2])

    def hop_send(e):
        return copy_to(5, xs.at[2, e, pl.ds(cap - HOP, HOP)], hop, xs_sem.at[0], hop_sem.at[0])

    def hop_on(e):
        return copy_to(4, hop, xr.at[2, e, pl.ds(cap - HOP, HOP)], hop_sem.at[1], xr_sem.at[2])

    def x_wait(i):
        at, places = pl.ds(*X_PIECES[i]), pl.ds(1, groups - 1)
        copy_to(1, xs.at[places, at], xr.at[places, at], xs_sem.at[0], xr_sem.at[i]).wait_recv()

    def y_send(i, p):
        at = pl.ds(*Y_PIECES[i])
        return copy_to(p, ys.at[p, at], yr.at[p, at], ys_sem.at[0], yr_sem.at[(0, 1, 2 + p // 2)[i]])

    def y_wait(i, first, count):
        at, places = pl.ds(*Y_PIECES[i]), pl.ds(first, count)
        copy_to(1, ys.at[places, at], yr.at[places, at], ys_sem.at[0], yr_sem.at[(0, 1, 2 + first // 2)[i]]).wait_recv()

    def end_send(p, first, count):
        at = pl.ds(first, count)
        return copy_to(p, ys.at[p, experts_here - 1, at], y_end.at[p - 4, at], ys_sem.at[0], yr_sem.at[4])

    def first_slot(e, p):
        return peer_of(me, ORDER[p]) * (experts_here * cap) + e * cap

    def block_hot(e, p):
        slot = lax.broadcasted_iota(jnp.int32, (cap, tokens), 0).astype(f32)
        taken = slot_of[pl.ds(peer_of(me, ORDER[p]) * experts_here + e, 1), :]
        return jnp.where(slot == taken, 1.0, 0.0).astype(bf16)

    for half in ((1, 2), (3, 0)):
        places = [2 * q + side for q in half for side in (0, 1)]
        for i, p in enumerate(places):
            dmat[i * cap:(i + 1) * cap, :] = block_hot(0, p)
        for n, part in enumerate(parts):
            if half[0] == 1:
                small[2 + n].wait()
            got = jnp.dot(dmat[0:4 * cap, :], tok[:, part], preferred_element_type=f32).astype(bf16)
            for i, p in enumerate(places):
                (xs if p else xr)[p, 0, :, part] = got[i * cap:(i + 1) * cap]
        if half[0] == 1:
            pl.semaphore_wait(barrier, 7)
        for p in places:
            if p:
                x_send(0, p).start()
    for e in range(2):
        wi_copy(e).start()
        wo_copy(e).start()

    def dispatch(e, _):
        for p in range(groups):
            dmat[p * cap:(p + 1) * cap, :] = block_hot(e, p)

        def columns(n, _):
            at = pl.ds(pl.multiple_of(n * blk, blk), blk)
            got = jnp.dot(dmat[...], tok[:, at], preferred_element_type=f32).astype(bf16)
            xs[:, e, :, at] = got.reshape(groups, cap, blk)
            return 0

        lax.fori_loop(0, dim // blk, columns, 0)
        @pl.when(e == 1)
        def _():
            for p in SENDS:
                x_send(1, p).start()

        @pl.when(e == 3)
        def _():
            @pl.when(me == 3)
            def _():
                hop_send(3).start()
                far_send(2, 0, cap).start()
                if HOP < cap:
                    far_send(3, 0, cap - HOP).start()

            @pl.when(me != 3)
            def _():
                x_send(2, 2).start()

            for p in SENDS[1:]:
                x_send(2, p).start()

        xr[0, e] = xs[0, e]
        return 0

    lax.fori_loop(1, experts_here, dispatch, 0)

    small[4].wait()
    logits = lax.dot_general(wg[...], tok[...], (((1,), (1,)), ((), ())), preferred_element_type=f32)
    top = jnp.max(logits, axis=0, keepdims=True)
    expd = jnp.exp(logits - top)
    probs = expd / jnp.sum(expd, axis=0, keepdims=True)
    id1, id2, kept2 = ids[0:1, :], ids[1:2, :], keep[0:1, :] > 0
    is1, is2 = expert_row == id1, (expert_row == id2) & kept2

    def pick(mask, value):
        return jnp.sum(jnp.where(mask, value, 0.0), axis=0, keepdims=True)

    gate1, gate2 = pick(is1, probs), pick(is2, probs)
    slot1, slot2 = pick(is1, slot_of[...]), pick(is2, slot_of[...])
    total = gate1 + gate2
    gates[0:1, :] = jnp.where(slot1 < cap, id1.astype(f32) * cap + slot1, -1.0)
    gates[1:2, :] = jnp.where((slot2 < cap) & kept2, id2.astype(f32) * cap + slot2, -1.0)
    gates[2:3, :] = gate1 / total
    gates[3:4, :] = gate2 / total
    gates[4:, :] = jnp.zeros((gates.shape[0] - 4, tokens), f32)
    cols[...] = gates[...].T

    for i, order in enumerate(CW_BLOCKS):
        lane = lax.broadcasted_iota(jnp.int32, (8, 2 * rows), 1)
        slot = lane
        for b, (p, e) in enumerate(order):
            slot = slot + jnp.where(lane // cap == b, first_slot(e, p) - b * cap, 0)
        slots[i] = slot.astype(f32)

    def weights(i, _):
        def block(t, _):
            at = pl.ds(pl.multiple_of(t * blk, blk), blk)
            slot = slots[i, 0:1, :]
            part = cols[at, :]
            cw[i, at, :] = (
                jnp.where(slot == part[:, 0:1], part[:, 2:3], 0.0) + jnp.where(slot == part[:, 1:2], part[:, 3:4], 0.0)
            ).astype(bf16)
            return 0

        return lax.fori_loop(0, tokens // blk, block, 0)

    lax.fori_loop(0, experts_here // 2, weights, 0)

    def expert(e, _):
        s = e % 2
        for i, (start, _count) in enumerate(X_PIECES):
            @pl.when(e == start)
            def _():
                x_wait(i)

        wi_copy(e).wait()

        @pl.when((e == 1) & (me == 7))
        def _():
            hop_send(3).wait_recv()
            hop_on(3).start()

        def up(j, _):
            at = pl.ds(pl.multiple_of(j * blk, blk), blk)
            pre = jnp.dot(xr[:, e].reshape(rows, dim), wi[s, :, at], preferred_element_type=f32)
            hid[:, at] = jnp.maximum(pre, 0.0).astype(bf16)
            return 0

        lax.fori_loop(0, hidden // blk, up, 0)

        @pl.when(e + 2 < experts_here)
        def _():
            wi_copy(e + 2).start()

        wo_copy(e).wait()

        def down(n, _):
            at = pl.ds(pl.multiple_of(n * blk, blk), blk)
            got = jnp.dot(hid[...], wo[s, :, at], preferred_element_type=f32).astype(bf16)
            ys[:, e, :, at] = got.reshape(groups, cap, blk)
            return 0

        lax.fori_loop(0, dim // blk, down, 0)

        @pl.when(e + 2 < experts_here)
        def _():
            wo_copy(e + 2).start()

        @pl.when(e == 1)
        def _():
            for p in SENDS:
                y_send(0, p).start()

        @pl.when(e == 2)
        def _():
            for p in NEAR:
                y_send(1, p).start()

        @pl.when(e == 3)
        def _():
            for p in FAR:
                y_send(2, p).start()

        @pl.when((e == 3) & (me % 2 == 0))
        def _():
            for p in NEAR:
                end_send(p, 0, cap).start()

        @pl.when((e == 3) & (me % 2 == 1))
        def _():
            for p, first, count in [(p, 0, cap - HELD) for p in (4, 5)] + [(p, 0, cap) for p in (6, 7)] + [(p, cap - HELD, HELD) for p in (4, 5)]:
                end_send(p, first, count).start()

        yr[0, e] = ys[0, e]
        return 0

    lax.fori_loop(0, experts_here, expert, 0)

    y_wait(0, 1, groups - 1)

    def columns(n, _):
        at = pl.ds(pl.multiple_of(n * blk, blk), blk)
        acc[:, at] = jnp.dot(cw[0], yr[:, 0:2, :, at].reshape(2 * rows, blk), preferred_element_type=f32)
        return 0

    lax.fori_loop(0, dim // blk, columns, 0)
    def add_rows(first, back_of):
        def part(n, _):
            at = pl.ds(pl.multiple_of(n * blk, blk), blk)
            acc[:, at] += jnp.dot(cw[1, :, first:first + 4 * cap], back_of(at).reshape(4 * cap, blk), preferred_element_type=f32)
            return 0

        lax.fori_loop(0, dim // blk, part, 0)

    y_wait(1, 4, 4)
    add_rows(rows, lambda at: yr[4:8, 2, :, at])
    y_wait(2, 1, 1)
    add_rows(0, lambda at: yr[0:2, 2:4, :, at])
    y_wait(2, 2, 2)
    add_rows(4 * cap, lambda at: yr[2:4, 2:4, :, at])
    cw_end[...] = cw[1, :, 2 * rows - 4 * cap:]
    @pl.when(me == 7)
    def _():
        hop_on(3).wait_send()

    sent = pl.ds(1, groups - 1)
    copy_to(1, xs.at[sent], xr.at[sent], xs_sem.at[0], xr_sem.at[0]).wait_send()
    copy_to(1, ys.at[4:8, 0], y_end, ys_sem.at[0], yr_sem.at[4]).wait_recv()
    copy_to(1, ys.at[sent], yr.at[sent], ys_sem.at[0], yr_sem.at[0]).wait_send()


def finish_kernel(acc, cw, y, out, buf, sem):
    blk = buf.shape[0] // 8
    for t in range(8):
        at = pl.ds(t * blk, blk)
        buf[at, :] = (acc[at, :] + jnp.dot(cw[at, :], y[...].reshape(cw.shape[1], acc.shape[1]), preferred_element_type=jnp.float32)).astype(out.dtype)
        pltpu.make_async_copy(buf.at[at], out.at[at], sem.at[0]).start()
    pltpu.make_async_copy(buf, out, sem.at[0]).wait()


def solution(mesh):
    def local_layer(tokens, w_gate, expert_ids, keep_second, w_in, w_out):
        _, token_count, dim = tokens.shape
        experts = w_gate.shape[1]
        here, _, hidden = w_in.shape
        cap = 2 * token_count // experts
        groups = experts // here
        rows = groups * cap
        f32, bf16 = jnp.float32, jnp.bfloat16
        vmem, dma = pltpu.VMEM, pltpu.SemaphoreType.DMA
        acc, cw_end, y_end = pl.pallas_call(
            functools.partial(layer_kernel, cap),
            out_shape=(vmem((token_count, dim), f32), vmem((token_count, 4 * cap), bf16), vmem((4, cap, dim), bf16)),
            in_specs=[pl.BlockSpec(memory_space=pl.ANY)] * 6,
            out_specs=[pl.BlockSpec(memory_space=vmem)] * 3,
            scratch_shapes=[
                vmem((token_count, dim), bf16),
                vmem((experts, dim), bf16),
                vmem((2, token_count), jnp.int32),
                vmem((1, token_count), jnp.int32),
                vmem((experts, token_count), f32),
                vmem((128, token_count), f32),
                vmem((token_count, 128), f32),
                vmem((2, 8, 2 * rows), f32),
                vmem((HOP, dim), bf16),
                vmem((rows, token_count), bf16),
                vmem((groups, here, cap, dim), bf16),
                vmem((groups, here, cap, dim), bf16),
                vmem((groups, here, cap, dim), bf16),
                vmem((groups, here, cap, dim), bf16),
                vmem((rows, hidden), bf16),
                vmem((2, dim, hidden), bf16),
                vmem((2, hidden, dim), bf16),
                vmem((here // 2, token_count, 2 * rows), bf16),
                dma((5,)), dma((2,)), dma((2,)),
                dma((1,)), dma((3,)), dma((1,)), dma((5,)), dma((2,)),
            ],
            compiler_params=pltpu.CompilerParams(collective_id=0, has_side_effects=True, vmem_limit_bytes=56 * 2**20),
            name="moe_layer",
        )(tokens[0], w_gate.T, expert_ids[0].T, keep_second, w_in, w_out)
        out = pl.pallas_call(
            finish_kernel,
            out_shape=jax.ShapeDtypeStruct((token_count, dim), bf16),
            in_specs=[pl.BlockSpec(memory_space=vmem)] * 3,
            out_specs=pl.BlockSpec(memory_space=pl.ANY),
            scratch_shapes=[vmem((token_count, dim), bf16), dma((1,))],
            compiler_params=pltpu.CompilerParams(vmem_limit_bytes=8 * 2**20),
            name="moe_finish",
        )(acc, cw_end, y_end)
        return out[None]

    group_spec = P(("dp", "ep"))
    return jax.shard_map(local_layer, mesh=mesh, in_specs=(group_spec, P(), group_spec, group_spec, P("ep"), P("ep")), out_specs=group_spec, check_vma=False)
```

```python
import functools

import jax
import jax.numpy as jnp
from jax import lax
from jax.experimental import pallas as pl
from jax.experimental.pallas import tpu as pltpu
from jax.sharding import PartitionSpec as P

MESH = pl.DeviceIdType.MESH
ORDER = (0, 1, 6, 7, 2, 4, 3, 5)
SENDS = (2, 3, 4, 5, 6, 7, 1)
X_PIECES = ((0, 1), (1, 1), (2, 2))
Y_PIECES = ((0, 2), (2, 1), (2, 2))
NEAR, FAR = (4, 5, 6, 7), (2, 3, 1)
HELD = 16
HOP = 16
CW_BLOCKS = (
    tuple((p, e) for p in range(8) for e in (0, 1)),
    tuple((p, e) for p in range(4) for e in (2, 3)) + tuple((p, e) for e in (2, 3) for p in NEAR),
)


def peer_of(me, k):
    core, x, y = me % 2, (me // 2) % 2, me // 4
    core_bit, x_bit, y_bit = k % 2, (k // 2) % 2, k // 4
    core = 1 - core if core_bit else core
    x = 1 - x if x_bit else x
    y = 1 - y if y_bit else y
    return (y * 2 + x) * 2 + core


def layer_kernel(
    cap, tok_hbm, wg_hbm, ids_hbm, keep_hbm, win_hbm, wout_hbm, acc, cw_end, y_end,
    tok, wg, ids, keep, slot_of, gates, cols, slots, hop, dmat, xs, xr, ys, yr, hid, wi, wo, cw,
    in_sem, wi_sem, wo_sem, xs_sem, xr_sem, ys_sem, yr_sem, hop_sem,
):
    me = lax.axis_index("ep")
    experts_here = win_hbm.shape[0]
    tokens, dim = tok.shape
    experts = wg.shape[0]
    hidden = hid.shape[1]
    groups = experts // experts_here
    rows = groups * cap
    f32, bf16 = jnp.float32, jnp.bfloat16

    parts = (pl.ds(0, dim // 2), pl.ds(dim // 2, dim // 2))
    small = [
        pltpu.make_async_copy(ids_hbm, ids, in_sem.at[0]),
        pltpu.make_async_copy(keep_hbm, keep, in_sem.at[1]),
    ] + [
        pltpu.make_async_copy(tok_hbm.at[:, part], tok.at[:, part], wi_sem.at[i]) for i, part in enumerate(parts)
    ] + [pltpu.make_async_copy(wg_hbm, wg, in_sem.at[2])]
    for copy in small:
        copy.start()

    barrier = pltpu.get_barrier_semaphore()
    for k in range(1, 8):
        pl.semaphore_signal(barrier, inc=1, device_id={"ep": peer_of(me, k)}, device_id_type=MESH)

    def wi_copy(e):
        return pltpu.make_async_copy(win_hbm.at[e], wi.at[e % 2], wi_sem.at[e % 2])

    def wo_copy(e):
        return pltpu.make_async_copy(wout_hbm.at[e], wo.at[e % 2], wo_sem.at[e % 2])

    blk = 256
    r_io = lax.broadcasted_iota(jnp.int32, (blk, blk), 0)
    c_io = lax.broadcasted_iota(jnp.int32, (blk, blk), 1)
    before = jnp.where(r_io < c_io, 1.0, 0.0).astype(bf16)
    ones = jnp.ones((blk, blk), bf16)
    expert_row = lax.broadcasted_iota(jnp.int32, (experts, tokens), 0)
    small[0].wait()
    small[1].wait()
    hot1 = (expert_row == ids[0:1, :]).astype(f32)
    hot2 = ((expert_row == ids[1:2, :]) & (keep[0:1, :] > 0)).astype(f32)
    hot = jnp.concatenate([hot1, hot2], axis=0).astype(bf16)
    blocks = range(tokens // blk)
    stack = jnp.concatenate([hot[:, b * blk:(b + 1) * blk] for b in blocks], axis=0)
    within = jnp.dot(stack, before, preferred_element_type=f32)
    counts = jnp.dot(stack, ones, preferred_element_type=f32)
    both = 2 * experts
    first_total = sum(counts[b * both:b * both + experts] for b in blocks)
    seen = jnp.zeros((both, blk), f32)
    for b in blocks:
        at = slice(b * blk, (b + 1) * blk)
        earlier = within[b * both:(b + 1) * both] + seen
        seen = seen + counts[b * both:(b + 1) * both]
        second = jnp.where(hot2[:, at] > 0, earlier[experts:] + first_total, -1.0)
        slot_of[:, at] = jnp.where(hot1[:, at] > 0, earlier[:experts], second)

    def copy_to(p, src, dst, send_sem, recv_sem):
        return pltpu.make_async_remote_copy(
            src_ref=src, dst_ref=dst, send_sem=send_sem, recv_sem=recv_sem,
            device_id={"ep": peer_of(me, ORDER[p])}, device_id_type=MESH,
        )

    def x_send(i, p):
        at = pl.ds(*X_PIECES[i])
        return copy_to(p, xs.at[p, at], xr.at[p, at], xs_sem.at[0], xr_sem.at[i])

    def far_send(e, first, count):
        at = pl.ds(first, count)
        return copy_to(2, xs.at[2, e, at], xr.at[2, e, at], xs_sem.at[0], xr_sem.at[2])

    def hop_send(e):
        return copy_to(5, xs.at[2, e, pl.ds(cap - HOP, HOP)], hop, xs_sem.at[0], hop_sem.at[0])

    def hop_on(e):
        return copy_to(4, hop, xr.at[2, e, pl.ds(cap - HOP, HOP)], hop_sem.at[1], xr_sem.at[2])

    def x_wait(i):
        at, places = pl.ds(*X_PIECES[i]), pl.ds(1, groups - 1)
        copy_to(1, xs.at[places, at], xr.at[places, at], xs_sem.at[0], xr_sem.at[i]).wait_recv()

    def y_send(i, p):
        at = pl.ds(*Y_PIECES[i])
        return copy_to(p, ys.at[p, at], yr.at[p, at], ys_sem.at[0], yr_sem.at[i])

    def y_wait(i, first, count):
        at, places = pl.ds(*Y_PIECES[i]), pl.ds(first, count)
        copy_to(1, ys.at[places, at], yr.at[places, at], ys_sem.at[0], yr_sem.at[i]).wait_recv()

    def end_send(p, first, count):
        at = pl.ds(first, count)
        return copy_to(p, ys.at[p, experts_here - 1, at], y_end.at[p - 4, at], ys_sem.at[0], yr_sem.at[3])

    def first_slot(e, p):
        return peer_of(me, ORDER[p]) * (experts_here * cap) + e * cap

    def block_hot(e, p):
        slot = lax.broadcasted_iota(jnp.int32, (cap, tokens), 0).astype(f32)
        taken = slot_of[pl.ds(peer_of(me, ORDER[p]) * experts_here + e, 1), :]
        return jnp.where(slot == taken, 1.0, 0.0).astype(bf16)

    for half in ((1, 2), (3, 0)):
        places = [2 * q + side for q in half for side in (0, 1)]
        for i, p in enumerate(places):
            dmat[i * cap:(i + 1) * cap, :] = block_hot(0, p)
        for n, part in enumerate(parts):
            if half[0] == 1:
                small[2 + n].wait()
            got = jnp.dot(dmat[0:4 * cap, :], tok[:, part], preferred_element_type=f32).astype(bf16)
            for i, p in enumerate(places):
                (xs if p else xr)[p, 0, :, part] = got[i * cap:(i + 1) * cap]
        if half[0] == 1:
            pl.semaphore_wait(barrier, 7)
        for p in places:
            if p:
                x_send(0, p).start()
    for e in range(2):
        wi_copy(e).start()
        wo_copy(e).start()

    def dispatch(e, _):
        for p in range(groups):
            dmat[p * cap:(p + 1) * cap, :] = block_hot(e, p)

        def columns(n, _):
            at = pl.ds(pl.multiple_of(n * blk, blk), blk)
            got = jnp.dot(dmat[...], tok[:, at], preferred_element_type=f32).astype(bf16)
            xs[:, e, :, at] = got.reshape(groups, cap, blk)
            return 0

        lax.fori_loop(0, dim // blk, columns, 0)
        @pl.when(e == 1)
        def _():
            for p in SENDS:
                x_send(1, p).start()

        @pl.when(e == 3)
        def _():
            @pl.when(me == 3)
            def _():
                hop_send(3).start()
                far_send(2, 0, cap).start()
                if HOP < cap:
                    far_send(3, 0, cap - HOP).start()

            @pl.when(me != 3)
            def _():
                x_send(2, 2).start()

            for p in SENDS[1:]:
                x_send(2, p).start()

        xr[0, e] = xs[0, e]
        return 0

    lax.fori_loop(1, experts_here, dispatch, 0)

    small[4].wait()
    logits = lax.dot_general(wg[...], tok[...], (((1,), (1,)), ((), ())), preferred_element_type=f32)
    top = jnp.max(logits, axis=0, keepdims=True)
    expd = jnp.exp(logits - top)
    probs = expd / jnp.sum(expd, axis=0, keepdims=True)
    id1, id2, kept2 = ids[0:1, :], ids[1:2, :], keep[0:1, :] > 0
    is1, is2 = expert_row == id1, (expert_row == id2) & kept2

    def pick(mask, value):
        return jnp.sum(jnp.where(mask, value, 0.0), axis=0, keepdims=True)

    gate1, gate2 = pick(is1, probs), pick(is2, probs)
    slot1, slot2 = pick(is1, slot_of[...]), pick(is2, slot_of[...])
    total = gate1 + gate2
    gates[0:1, :] = jnp.where(slot1 < cap, id1.astype(f32) * cap + slot1, -1.0)
    gates[1:2, :] = jnp.where((slot2 < cap) & kept2, id2.astype(f32) * cap + slot2, -1.0)
    gates[2:3, :] = gate1 / total
    gates[3:4, :] = gate2 / total
    gates[4:, :] = jnp.zeros((gates.shape[0] - 4, tokens), f32)
    cols[...] = gates[...].T

    for i, order in enumerate(CW_BLOCKS):
        lane = lax.broadcasted_iota(jnp.int32, (8, 2 * rows), 1)
        slot = lane
        for b, (p, e) in enumerate(order):
            slot = slot + jnp.where(lane // cap == b, first_slot(e, p) - b * cap, 0)
        slots[i] = slot.astype(f32)

    def weights(i, _):
        def block(t, _):
            at = pl.ds(pl.multiple_of(t * blk, blk), blk)
            slot = slots[i, 0:1, :]
            part = cols[at, :]
            cw[i, at, :] = (
                jnp.where(slot == part[:, 0:1], part[:, 2:3], 0.0) + jnp.where(slot == part[:, 1:2], part[:, 3:4], 0.0)
            ).astype(bf16)
            return 0

        return lax.fori_loop(0, tokens // blk, block, 0)

    lax.fori_loop(0, experts_here // 2, weights, 0)

    def expert(e, _):
        s = e % 2
        for i, (start, _count) in enumerate(X_PIECES):
            @pl.when(e == start)
            def _():
                x_wait(i)

        wi_copy(e).wait()

        @pl.when((e == 1) & (me == 7))
        def _():
            hop_send(3).wait_recv()
            hop_on(3).start()

        def up(j, _):
            at = pl.ds(pl.multiple_of(j * blk, blk), blk)
            pre = jnp.dot(xr[:, e].reshape(rows, dim), wi[s, :, at], preferred_element_type=f32)
            hid[:, at] = jnp.maximum(pre, 0.0).astype(bf16)
            return 0

        lax.fori_loop(0, hidden // blk, up, 0)

        @pl.when(e + 2 < experts_here)
        def _():
            wi_copy(e + 2).start()

        wo_copy(e).wait()

        def down(n, _):
            at = pl.ds(pl.multiple_of(n * blk, blk), blk)
            got = jnp.dot(hid[...], wo[s, :, at], preferred_element_type=f32).astype(bf16)
            ys[:, e, :, at] = got.reshape(groups, cap, blk)
            return 0

        lax.fori_loop(0, dim // blk, down, 0)

        @pl.when(e + 2 < experts_here)
        def _():
            wo_copy(e + 2).start()

        @pl.when(e == 1)
        def _():
            for p in SENDS:
                y_send(0, p).start()

        @pl.when(e == 2)
        def _():
            for p in NEAR:
                y_send(1, p).start()

        @pl.when(e == 3)
        def _():
            for p in FAR:
                y_send(2, p).start()

        @pl.when((e == 3) & (me % 2 == 0))
        def _():
            for p in NEAR:
                end_send(p, 0, cap).start()

        @pl.when((e == 3) & (me % 2 == 1))
        def _():
            for p, first, count in [(p, 0, cap - HELD) for p in (4, 5)] + [(p, 0, cap) for p in (6, 7)] + [(p, cap - HELD, HELD) for p in (4, 5)]:
                end_send(p, first, count).start()

        yr[0, e] = ys[0, e]
        return 0

    lax.fori_loop(0, experts_here, expert, 0)

    y_wait(0, 1, groups - 1)

    def columns(n, _):
        at = pl.ds(pl.multiple_of(n * blk, blk), blk)
        acc[:, at] = jnp.dot(cw[0], yr[:, 0:2, :, at].reshape(2 * rows, blk), preferred_element_type=f32)
        return 0

    lax.fori_loop(0, dim // blk, columns, 0)
    def add_rows(first, back_of):
        def part(n, _):
            at = pl.ds(pl.multiple_of(n * blk, blk), blk)
            acc[:, at] += jnp.dot(cw[1, :, first:first + 4 * cap], back_of(at).reshape(4 * cap, blk), preferred_element_type=f32)
            return 0

        lax.fori_loop(0, dim // blk, part, 0)

    y_wait(1, 4, 4)
    add_rows(rows, lambda at: yr[4:8, 2, :, at])
    y_wait(2, 1, 3)
    add_rows(0, lambda at: yr[0:2, 2:4, :, at])
    add_rows(4 * cap, lambda at: yr[2:4, 2:4, :, at])
    cw_end[...] = cw[1, :, 2 * rows - 4 * cap:]
    @pl.when(me == 7)
    def _():
        hop_on(3).wait_send()

    sent = pl.ds(1, groups - 1)
    copy_to(1, xs.at[sent], xr.at[sent], xs_sem.at[0], xr_sem.at[0]).wait_send()
    copy_to(1, ys.at[4:8, 0], y_end, ys_sem.at[0], yr_sem.at[3]).wait_recv()
    copy_to(1, ys.at[sent], yr.at[sent], ys_sem.at[0], yr_sem.at[0]).wait_send()


def finish_kernel(acc, cw, y, out, buf, sem):
    blk = buf.shape[0] // 8
    for t in range(8):
        at = pl.ds(t * blk, blk)
        buf[at, :] = (acc[at, :] + jnp.dot(cw[at, :], y[...].reshape(cw.shape[1], acc.shape[1]), preferred_element_type=jnp.float32)).astype(out.dtype)
        pltpu.make_async_copy(buf.at[at], out.at[at], sem.at[0]).start()
    pltpu.make_async_copy(buf, out, sem.at[0]).wait()


def solution(mesh):
    def local_layer(tokens, w_gate, expert_ids, keep_second, w_in, w_out):
        _, token_count, dim = tokens.shape
        experts = w_gate.shape[1]
        here, _, hidden = w_in.shape
        cap = 2 * token_count // experts
        groups = experts // here
        rows = groups * cap
        f32, bf16 = jnp.float32, jnp.bfloat16
        vmem, dma = pltpu.VMEM, pltpu.SemaphoreType.DMA
        acc, cw_end, y_end = pl.pallas_call(
            functools.partial(layer_kernel, cap),
            out_shape=(vmem((token_count, dim), f32), vmem((token_count, 4 * cap), bf16), vmem((4, cap, dim), bf16)),
            in_specs=[pl.BlockSpec(memory_space=pl.ANY)] * 6,
            out_specs=[pl.BlockSpec(memory_space=vmem)] * 3,
            scratch_shapes=[
                vmem((token_count, dim), bf16),
                vmem((experts, dim), bf16),
                vmem((2, token_count), jnp.int32),
                vmem((1, token_count), jnp.int32),
                vmem((experts, token_count), f32),
                vmem((128, token_count), f32),
                vmem((token_count, 128), f32),
                vmem((2, 8, 2 * rows), f32),
                vmem((HOP, dim), bf16),
                vmem((rows, token_count), bf16),
                vmem((groups, here, cap, dim), bf16),
                vmem((groups, here, cap, dim), bf16),
                vmem((groups, here, cap, dim), bf16),
                vmem((groups, here, cap, dim), bf16),
                vmem((rows, hidden), bf16),
                vmem((2, dim, hidden), bf16),
                vmem((2, hidden, dim), bf16),
                vmem((here // 2, token_count, 2 * rows), bf16),
                dma((3,)), dma((2,)), dma((2,)),
                dma((1,)), dma((3,)), dma((1,)), dma((4,)), dma((2,)),
            ],
            compiler_params=pltpu.CompilerParams(collective_id=0, has_side_effects=True, vmem_limit_bytes=56 * 2**20),
            name="moe_layer",
        )(tokens[0], w_gate.T, expert_ids[0].T, keep_second, w_in, w_out)
        out = pl.pallas_call(
            finish_kernel,
            out_shape=jax.ShapeDtypeStruct((token_count, dim), bf16),
            in_specs=[pl.BlockSpec(memory_space=vmem)] * 3,
            out_specs=pl.BlockSpec(memory_space=pl.ANY),
            scratch_shapes=[vmem((token_count, dim), bf16), dma((1,))],
            compiler_params=pltpu.CompilerParams(vmem_limit_bytes=8 * 2**20),
            name="moe_finish",
        )(acc, cw_end, y_end)
        return out[None]

    group_spec = P(("dp", "ep"))
    return jax.shard_map(local_layer, mesh=mesh, in_specs=(group_spec, P(), group_spec, group_spec, P("ep"), P("ep")), out_specs=group_spec, check_vma=False)
```

```python
import functools

import jax
import jax.numpy as jnp
from jax import lax
from jax.experimental import pallas as pl
from jax.experimental.pallas import tpu as pltpu
from jax.sharding import PartitionSpec as P

MESH = pl.DeviceIdType.MESH
ORDER = (0, 1, 6, 7, 2, 4, 3, 5)
SENDS = (2, 4, 5, 3, 6, 7, 1)
X_PIECES = ((0, 1), (1, 1), (2, 2))
Y_PIECES = ((0, 2), (2, 1), (2, 2))
NEAR, FAR = (4, 5, 6, 7), (2, 3, 1)
HELD = 16
HOP = 16
CW_BLOCKS = (
    tuple((p, e) for p in range(8) for e in (0, 1)),
    tuple((p, e) for p in range(4) for e in (2, 3)) + tuple((p, e) for e in (2, 3) for p in NEAR),
)


def peer_of(me, k):
    core, x, y = me % 2, (me // 2) % 2, me // 4
    core_bit, x_bit, y_bit = k % 2, (k // 2) % 2, k // 4
    core = 1 - core if core_bit else core
    x = 1 - x if x_bit else x
    y = 1 - y if y_bit else y
    return (y * 2 + x) * 2 + core


def layer_kernel(
    cap, tok_hbm, wg_hbm, ids_hbm, keep_hbm, win_hbm, wout_hbm, acc, cw_end, y_end,
    tok, wg, ids, keep, slot_of, gates, cols, slots, hop, dmat, out_rows, xr, yr, hid, wi, wo, cw,
    in_sem, wi_sem, wo_sem, sent_sem, xr_sem, yr_sem, hop_sem,
):
    me = lax.axis_index("ep")
    xs, ys = out_rows.at[0], out_rows.at[1]
    experts_here = win_hbm.shape[0]
    tokens, dim = tok.shape
    experts = wg.shape[0]
    hidden = hid.shape[1]
    groups = experts // experts_here
    rows = groups * cap
    f32, bf16 = jnp.float32, jnp.bfloat16

    parts = (pl.ds(0, dim // 2), pl.ds(dim // 2, dim // 2))
    small = [
        pltpu.make_async_copy(ids_hbm, ids, in_sem.at[0]),
        pltpu.make_async_copy(keep_hbm, keep, in_sem.at[1]),
    ] + [
        pltpu.make_async_copy(tok_hbm.at[:, part], tok.at[:, part], wi_sem.at[i]) for i, part in enumerate(parts)
    ] + [pltpu.make_async_copy(wg_hbm, wg, in_sem.at[2])]
    for copy in small:
        copy.start()

    barrier = pltpu.get_barrier_semaphore()
    for k in range(1, 8):
        pl.semaphore_signal(barrier, inc=1, device_id={"ep": peer_of(me, k)}, device_id_type=MESH)

    def wi_copy(e):
        return pltpu.make_async_copy(win_hbm.at[e], wi.at[e % 2], wi_sem.at[e % 2])

    def wo_copy(e):
        return pltpu.make_async_copy(wout_hbm.at[e], wo.at[e % 2], wo_sem.at[e % 2])

    blk = 256
    r_io = lax.broadcasted_iota(jnp.int32, (blk, blk), 0)
    c_io = lax.broadcasted_iota(jnp.int32, (blk, blk), 1)
    before = jnp.where(r_io < c_io, 1.0, 0.0).astype(bf16)
    ones = jnp.ones((blk, blk), bf16)
    expert_row = lax.broadcasted_iota(jnp.int32, (experts, tokens), 0)
    small[0].wait()
    small[1].wait()
    hot1 = (expert_row == ids[0:1, :]).astype(f32)
    hot2 = ((expert_row == ids[1:2, :]) & (keep[0:1, :] > 0)).astype(f32)
    hot = jnp.concatenate([hot1, hot2], axis=0).astype(bf16)
    blocks = range(tokens // blk)
    stack = jnp.concatenate([hot[:, b * blk:(b + 1) * blk] for b in blocks], axis=0)
    within = jnp.dot(stack, before, preferred_element_type=f32)
    counts = jnp.dot(stack, ones, preferred_element_type=f32)
    both = 2 * experts
    first_total = sum(counts[b * both:b * both + experts] for b in blocks)
    seen = jnp.zeros((both, blk), f32)
    for b in blocks:
        at = slice(b * blk, (b + 1) * blk)
        earlier = within[b * both:(b + 1) * both] + seen
        seen = seen + counts[b * both:(b + 1) * both]
        second = jnp.where(hot2[:, at] > 0, earlier[experts:] + first_total, -1.0)
        slot_of[:, at] = jnp.where(hot1[:, at] > 0, earlier[:experts], second)

    def copy_to(p, src, dst, send_sem, recv_sem):
        return pltpu.make_async_remote_copy(
            src_ref=src, dst_ref=dst, send_sem=send_sem, recv_sem=recv_sem,
            device_id={"ep": peer_of(me, ORDER[p])}, device_id_type=MESH,
        )

    def x_send(i, p):
        at = pl.ds(*X_PIECES[i])
        return copy_to(p, xs.at[p, at], xr.at[p, at], sent_sem.at[0], xr_sem.at[i])

    def far_send(e, first, count):
        at = pl.ds(first, count)
        return copy_to(2, xs.at[2, e, at], xr.at[2, e, at], sent_sem.at[0], xr_sem.at[2])

    def hop_send(e):
        return copy_to(5, xs.at[2, e, pl.ds(cap - HOP, HOP)], hop, sent_sem.at[0], hop_sem.at[0])

    def hop_on(e):
        return copy_to(4, hop, xr.at[2, e, pl.ds(cap - HOP, HOP)], hop_sem.at[1], xr_sem.at[2])

    def x_wait(i):
        at, places = pl.ds(*X_PIECES[i]), pl.ds(1, groups - 1)
        copy_to(1, xs.at[places, at], xr.at[places, at], sent_sem.at[0], xr_sem.at[i]).wait_recv()

    def y_send(i, p):
        at = pl.ds(*Y_PIECES[i])
        return copy_to(p, ys.at[p, at], yr.at[p, at], sent_sem.at[0], yr_sem.at[i])

    def y_wait(i, first, count):
        at, places = pl.ds(*Y_PIECES[i]), pl.ds(first, count)
        copy_to(1, ys.at[places, at], yr.at[places, at], sent_sem.at[0], yr_sem.at[i]).wait_recv()

    def end_send(p, first, count):
        at = pl.ds(first, count)
        return copy_to(p, ys.at[p, experts_here - 1, at], y_end.at[p - 4, at], sent_sem.at[0], yr_sem.at[3])

    def first_slot(e, p):
        return peer_of(me, ORDER[p]) * (experts_here * cap) + e * cap

    def block_hot(e, p):
        slot = lax.broadcasted_iota(jnp.int32, (cap, tokens), 0).astype(f32)
        taken = slot_of[pl.ds(peer_of(me, ORDER[p]) * experts_here + e, 1), :]
        return jnp.where(slot == taken, 1.0, 0.0).astype(bf16)

    for half in ((1, 2), (3, 0)):
        places = [2 * q + side for q in half for side in (0, 1)]
        for i, p in enumerate(places):
            dmat[i * cap:(i + 1) * cap, :] = block_hot(0, p)
        for n, part in enumerate(parts):
            if half[0] == 1:
                small[2 + n].wait()
            got = jnp.dot(dmat[0:4 * cap, :], tok[:, part], preferred_element_type=f32).astype(bf16)
            for i, p in enumerate(places):
                (xs if p else xr)[p, 0, :, part] = got[i * cap:(i + 1) * cap]
        if half[0] == 1:
            pl.semaphore_wait(barrier, 7)
        for p in places:
            if p:
                x_send(0, p).start()
    for e in range(2):
        wi_copy(e).start()
        wo_copy(e).start()

    def dispatch(e, _):
        for p in range(groups):
            dmat[p * cap:(p + 1) * cap, :] = block_hot(e, p)

        def columns(n, _):
            at = pl.ds(pl.multiple_of(n * blk, blk), blk)
            got = jnp.dot(dmat[...], tok[:, at], preferred_element_type=f32).astype(bf16)
            xs[:, e, :, at] = got.reshape(groups, cap, blk)
            return 0

        lax.fori_loop(0, dim // blk, columns, 0)
        @pl.when(e == 1)
        def _():
            for p in SENDS:
                x_send(1, p).start()

        @pl.when(e == 3)
        def _():
            @pl.when(me == 3)
            def _():
                hop_send(3).start()
                far_send(2, 0, cap).start()
                if HOP < cap:
                    far_send(3, 0, cap - HOP).start()

            @pl.when(me != 3)
            def _():
                x_send(2, 2).start()

            for p in SENDS[1:]:
                x_send(2, p).start()

        xr[0, e] = xs[0, e]
        return 0

    lax.fori_loop(1, experts_here, dispatch, 0)

    small[4].wait()
    logits = lax.dot_general(wg[...], tok[...], (((1,), (1,)), ((), ())), preferred_element_type=f32)
    top = jnp.max(logits, axis=0, keepdims=True)
    expd = jnp.exp(logits - top)
    probs = expd / jnp.sum(expd, axis=0, keepdims=True)
    id1, id2, kept2 = ids[0:1, :], ids[1:2, :], keep[0:1, :] > 0
    is1, is2 = expert_row == id1, (expert_row == id2) & kept2

    def pick(mask, value):
        return jnp.sum(jnp.where(mask, value, 0.0), axis=0, keepdims=True)

    gate1, gate2 = pick(is1, probs), pick(is2, probs)
    slot1, slot2 = pick(is1, slot_of[...]), pick(is2, slot_of[...])
    total = gate1 + gate2
    gates[0:1, :] = jnp.where(slot1 < cap, id1.astype(f32) * cap + slot1, -1.0)
    gates[1:2, :] = jnp.where((slot2 < cap) & kept2, id2.astype(f32) * cap + slot2, -1.0)
    gates[2:3, :] = gate1 / total
    gates[3:4, :] = gate2 / total
    gates[4:, :] = jnp.zeros((gates.shape[0] - 4, tokens), f32)
    cols[...] = gates[...].T

    for i, order in enumerate(CW_BLOCKS):
        lane = lax.broadcasted_iota(jnp.int32, (8, 2 * rows), 1)
        slot = lane
        for b, (p, e) in enumerate(order):
            slot = slot + jnp.where(lane // cap == b, first_slot(e, p) - b * cap, 0)
        slots[i] = slot.astype(f32)

    def weights(i, _):
        def block(t, _):
            at = pl.ds(pl.multiple_of(t * blk, blk), blk)
            slot = slots[i, 0:1, :]
            part = cols[at, :]
            cw[i, at, :] = (
                jnp.where(slot == part[:, 0:1], part[:, 2:3], 0.0) + jnp.where(slot == part[:, 1:2], part[:, 3:4], 0.0)
            ).astype(bf16)
            return 0

        return lax.fori_loop(0, tokens // blk, block, 0)

    lax.fori_loop(0, experts_here // 2, weights, 0)

    def expert(e, _):
        s = e % 2
        for i, (start, _count) in enumerate(X_PIECES):
            @pl.when(e == start)
            def _():
                x_wait(i)

        wi_copy(e).wait()

        @pl.when((e == 1) & (me == 7))
        def _():
            hop_send(3).wait_recv()
            hop_on(3).start()

        def up(j, _):
            at = pl.ds(pl.multiple_of(j * blk, blk), blk)
            pre = jnp.dot(xr[:, e].reshape(rows, dim), wi[s, :, at], preferred_element_type=f32)
            hid[:, at] = jnp.maximum(pre, 0.0).astype(bf16)
            return 0

        lax.fori_loop(0, hidden // blk, up, 0)

        @pl.when(e + 2 < experts_here)
        def _():
            wi_copy(e + 2).start()

        wo_copy(e).wait()

        def down(n, _):
            at = pl.ds(pl.multiple_of(n * blk, blk), blk)
            got = jnp.dot(hid[...], wo[s, :, at], preferred_element_type=f32).astype(bf16)
            ys[:, e, :, at] = got.reshape(groups, cap, blk)
            return 0

        lax.fori_loop(0, dim // blk, down, 0)

        @pl.when(e + 2 < experts_here)
        def _():
            wo_copy(e + 2).start()

        @pl.when(e == 1)
        def _():
            for p in SENDS:
                y_send(0, p).start()

        @pl.when(e == 2)
        def _():
            for p in NEAR:
                y_send(1, p).start()

        @pl.when(e == 3)
        def _():
            for p in FAR:
                y_send(2, p).start()

        @pl.when((e == 3) & (me % 2 == 0))
        def _():
            for p in NEAR:
                end_send(p, 0, cap).start()

        @pl.when((e == 3) & (me % 2 == 1))
        def _():
            for p, first, count in [(p, 0, cap - HELD) for p in (4, 5)] + [(p, 0, cap) for p in (6, 7)] + [(p, cap - HELD, HELD) for p in (4, 5)]:
                end_send(p, first, count).start()

        yr[0, e] = ys[0, e]
        return 0

    lax.fori_loop(0, experts_here, expert, 0)

    y_wait(0, 1, groups - 1)

    def columns(n, _):
        at = pl.ds(pl.multiple_of(n * blk, blk), blk)
        acc[:, at] = jnp.dot(cw[0], yr[:, 0:2, :, at].reshape(2 * rows, blk), preferred_element_type=f32)
        return 0

    lax.fori_loop(0, dim // blk, columns, 0)
    def add_rows(first, back_of):
        def part(n, _):
            at = pl.ds(pl.multiple_of(n * blk, blk), blk)
            acc[:, at] += jnp.dot(cw[1, :, first:first + 4 * cap], back_of(at).reshape(4 * cap, blk), preferred_element_type=f32)
            return 0

        lax.fori_loop(0, dim // blk, part, 0)

    y_wait(1, 4, 4)
    add_rows(rows, lambda at: yr[4:8, 2, :, at])
    y_wait(2, 1, 3)
    add_rows(0, lambda at: yr[0:2, 2:4, :, at])
    add_rows(4 * cap, lambda at: yr[2:4, 2:4, :, at])
    cw_end[...] = cw[1, :, 2 * rows - 4 * cap:]
    @pl.when(me == 7)
    def _():
        hop_on(3).wait_send()

    sent = pl.ds(1, groups - 1)
    copy_to(1, ys.at[4:8, 0], y_end, sent_sem.at[0], yr_sem.at[3]).wait_recv()
    everything = out_rows.at[:, sent]
    copy_to(1, everything, everything, sent_sem.at[0], xr_sem.at[0]).wait_send()


def finish_kernel(acc, cw, y, out, buf, sem):
    blk = buf.shape[0] // 8
    for t in range(8):
        at = pl.ds(t * blk, blk)
        buf[at, :] = (acc[at, :] + jnp.dot(cw[at, :], y[...].reshape(cw.shape[1], acc.shape[1]), preferred_element_type=jnp.float32)).astype(out.dtype)
        pltpu.make_async_copy(buf.at[at], out.at[at], sem.at[0]).start()
    pltpu.make_async_copy(buf, out, sem.at[0]).wait()


def solution(mesh):
    def local_layer(tokens, w_gate, expert_ids, keep_second, w_in, w_out):
        _, token_count, dim = tokens.shape
        experts = w_gate.shape[1]
        here, _, hidden = w_in.shape
        cap = 2 * token_count // experts
        groups = experts // here
        rows = groups * cap
        f32, bf16 = jnp.float32, jnp.bfloat16
        vmem, dma = pltpu.VMEM, pltpu.SemaphoreType.DMA
        acc, cw_end, y_end = pl.pallas_call(
            functools.partial(layer_kernel, cap),
            out_shape=(vmem((token_count, dim), f32), vmem((token_count, 4 * cap), bf16), vmem((4, cap, dim), bf16)),
            in_specs=[pl.BlockSpec(memory_space=pl.ANY)] * 6,
            out_specs=[pl.BlockSpec(memory_space=vmem)] * 3,
            scratch_shapes=[
                vmem((token_count, dim), bf16),
                vmem((experts, dim), bf16),
                vmem((2, token_count), jnp.int32),
                vmem((1, token_count), jnp.int32),
                vmem((experts, token_count), f32),
                vmem((128, token_count), f32),
                vmem((token_count, 128), f32),
                vmem((2, 8, 2 * rows), f32),
                vmem((HOP, dim), bf16),
                vmem((rows, token_count), bf16),
                vmem((2, groups, here, cap, dim), bf16),
                vmem((groups, here, cap, dim), bf16),
                vmem((groups, here, cap, dim), bf16),
                vmem((rows, hidden), bf16),
                vmem((2, dim, hidden), bf16),
                vmem((2, hidden, dim), bf16),
                vmem((here // 2, token_count, 2 * rows), bf16),
                dma((3,)), dma((2,)), dma((2,)),
                dma((1,)), dma((3,)), dma((4,)), dma((2,)),
            ],
            compiler_params=pltpu.CompilerParams(collective_id=0, has_side_effects=True, vmem_limit_bytes=56 * 2**20),
            name="moe_layer",
        )(tokens[0], w_gate.T, expert_ids[0].T, keep_second, w_in, w_out)
        out = pl.pallas_call(
            finish_kernel,
            out_shape=jax.ShapeDtypeStruct((token_count, dim), bf16),
            in_specs=[pl.BlockSpec(memory_space=vmem)] * 3,
            out_specs=pl.BlockSpec(memory_space=pl.ANY),
            scratch_shapes=[vmem((token_count, dim), bf16), dma((1,))],
            compiler_params=pltpu.CompilerParams(vmem_limit_bytes=8 * 2**20),
            name="moe_finish",
        )(acc, cw_end, y_end)
        return out[None]

    group_spec = P(("dp", "ep"))
    return jax.shard_map(local_layer, mesh=mesh, in_specs=(group_spec, P(), group_spec, group_spec, P("ep"), P("ep")), out_specs=group_spec, check_vma=False)
```

```python
import functools

import jax
import jax.numpy as jnp
from jax import lax
from jax.experimental import pallas as pl
from jax.experimental.pallas import tpu as pltpu
from jax.sharding import PartitionSpec as P

MESH = pl.DeviceIdType.MESH
ORDER = (0, 1, 6, 7, 2, 4, 3, 5)
SENDS = (2, 4, 5, 3, 6, 7, 1)
X_PIECES = ((0, 1), (1, 1), (2, 2))
Y_PIECES = ((0, 2), (2, 1), (2, 2))
NEAR, FAR = (4, 5, 6, 7), (2, 3, 1)
HELD = 16
HOP = 16
CW_BLOCKS = (
    tuple((p, e) for p in range(8) for e in (0, 1)),
    tuple((p, e) for p in range(4) for e in (2, 3)) + tuple((p, e) for e in (2, 3) for p in NEAR),
)


def peer_of(me, k):
    core, x, y = me % 2, (me // 2) % 2, me // 4
    core_bit, x_bit, y_bit = k % 2, (k // 2) % 2, k // 4
    core = 1 - core if core_bit else core
    x = 1 - x if x_bit else x
    y = 1 - y if y_bit else y
    return (y * 2 + x) * 2 + core


def layer_kernel(
    cap, tok_hbm, wg_hbm, ids_hbm, keep_hbm, win_hbm, wout_hbm, acc, cw_end, y_end,
    tok, wg, ids, keep, slot_of, gates, cols, slots, hop, dmat, out_rows, xr, yr, hid, wi, wo, cw,
    in_sem, wi_sem, wo_sem, sent_sem, xr_sem, yr_sem, hop_sem,
):
    me = lax.axis_index("ep")
    xs, ys = out_rows.at[0], out_rows.at[1]
    experts_here = win_hbm.shape[0]
    tokens, dim = tok.shape
    experts = wg.shape[0]
    hidden = hid.shape[1]
    groups = experts // experts_here
    rows = groups * cap
    f32, bf16 = jnp.float32, jnp.bfloat16

    parts = (pl.ds(0, dim // 2), pl.ds(dim // 2, dim // 2))
    small = [
        pltpu.make_async_copy(ids_hbm, ids, in_sem.at[0]),
        pltpu.make_async_copy(keep_hbm, keep, in_sem.at[1]),
    ] + [
        pltpu.make_async_copy(tok_hbm.at[:, part], tok.at[:, part], wi_sem.at[i]) for i, part in enumerate(parts)
    ] + [pltpu.make_async_copy(wg_hbm, wg, in_sem.at[2])]
    for copy in small:
        copy.start()

    barrier = pltpu.get_barrier_semaphore()
    for k in range(1, 8):
        pl.semaphore_signal(barrier, inc=1, device_id={"ep": peer_of(me, k)}, device_id_type=MESH)

    def wi_copy(e):
        return pltpu.make_async_copy(win_hbm.at[e], wi.at[e % 2], wi_sem.at[e % 2])

    def wo_copy(e):
        return pltpu.make_async_copy(wout_hbm.at[e], wo.at[e % 2], wo_sem.at[e % 2])

    blk = 256
    r_io = lax.broadcasted_iota(jnp.int32, (blk, blk), 0)
    c_io = lax.broadcasted_iota(jnp.int32, (blk, blk), 1)
    before = jnp.where(r_io < c_io, 1.0, 0.0).astype(bf16)
    ones = jnp.ones((blk, blk), bf16)
    expert_row = lax.broadcasted_iota(jnp.int32, (experts, tokens), 0)
    small[0].wait()
    small[1].wait()
    hot1 = (expert_row == ids[0:1, :]).astype(f32)
    hot2 = ((expert_row == ids[1:2, :]) & (keep[0:1, :] > 0)).astype(f32)
    hot = jnp.concatenate([hot1, hot2], axis=0).astype(bf16)
    blocks = range(tokens // blk)
    stack = jnp.concatenate([hot[:, b * blk:(b + 1) * blk] for b in blocks], axis=0)
    within = jnp.dot(stack, before, preferred_element_type=f32)
    counts = jnp.dot(stack, ones, preferred_element_type=f32)
    both = 2 * experts
    first_total = sum(counts[b * both:b * both + experts] for b in blocks)
    seen = jnp.zeros((both, blk), f32)
    for b in blocks:
        at = slice(b * blk, (b + 1) * blk)
        earlier = within[b * both:(b + 1) * both] + seen
        seen = seen + counts[b * both:(b + 1) * both]
        second = jnp.where(hot2[:, at] > 0, earlier[experts:] + first_total, -1.0)
        slot_of[:, at] = jnp.where(hot1[:, at] > 0, earlier[:experts], second)

    def copy_to(p, src, dst, send_sem, recv_sem):
        return pltpu.make_async_remote_copy(
            src_ref=src, dst_ref=dst, send_sem=send_sem, recv_sem=recv_sem,
            device_id={"ep": peer_of(me, ORDER[p])}, device_id_type=MESH,
        )

    def x_send(i, p):
        at = pl.ds(*X_PIECES[i])
        return copy_to(p, xs.at[p, at], xr.at[p, at], sent_sem.at[0], xr_sem.at[i])

    def far_send(e, first, count):
        at = pl.ds(first, count)
        return copy_to(2, xs.at[2, e, at], xr.at[2, e, at], sent_sem.at[0], xr_sem.at[2])

    def hop_send(e):
        return copy_to(5, xs.at[2, e, pl.ds(cap - HOP, HOP)], hop, sent_sem.at[0], hop_sem.at[0])

    def hop_on(e):
        return copy_to(4, hop, xr.at[2, e, pl.ds(cap - HOP, HOP)], hop_sem.at[1], xr_sem.at[2])

    def x_wait(i):
        at, places = pl.ds(*X_PIECES[i]), pl.ds(1, groups - 1)
        copy_to(1, xs.at[places, at], xr.at[places, at], sent_sem.at[0], xr_sem.at[i]).wait_recv()

    def y_send(i, p):
        at = pl.ds(*Y_PIECES[i])
        return copy_to(p, ys.at[p, at], yr.at[p, at], sent_sem.at[0], yr_sem.at[i])

    def y_wait(i, first, count):
        at, places = pl.ds(*Y_PIECES[i]), pl.ds(first, count)
        copy_to(1, ys.at[places, at], yr.at[places, at], sent_sem.at[0], yr_sem.at[i]).wait_recv()

    def end_send(p, first, count):
        at = pl.ds(first, count)
        return copy_to(p, ys.at[p, experts_here - 1, at], y_end.at[p - 4, at], sent_sem.at[0], yr_sem.at[3])

    def first_slot(e, p):
        return peer_of(me, ORDER[p]) * (experts_here * cap) + e * cap

    def block_hot(e, p):
        slot = lax.broadcasted_iota(jnp.int32, (cap, tokens), 0).astype(f32)
        taken = slot_of[pl.ds(peer_of(me, ORDER[p]) * experts_here + e, 1), :]
        return jnp.where(slot == taken, 1.0, 0.0).astype(bf16)

    for half in ((1, 2), (3, 0)):
        places = [2 * q + side for q in half for side in (0, 1)]
        for i, p in enumerate(places):
            dmat[i * cap:(i + 1) * cap, :] = block_hot(0, p)
        for n, part in enumerate(parts):
            if half[0] == 1:
                small[2 + n].wait()
            got = jnp.dot(dmat[0:4 * cap, :], tok[:, part], preferred_element_type=f32).astype(bf16)
            for i, p in enumerate(places):
                (xs if p else xr)[p, 0, :, part] = got[i * cap:(i + 1) * cap]
        if half[0] == 1:
            pl.semaphore_wait(barrier, 7)
        for p in places:
            if p:
                x_send(0, p).start()
    for e in range(2):
        wi_copy(e).start()
        wo_copy(e).start()

    def dispatch(e, _):
        for p in range(groups):
            dmat[p * cap:(p + 1) * cap, :] = block_hot(e, p)

        def columns(n, _):
            at = pl.ds(pl.multiple_of(n * blk, blk), blk)
            got = jnp.dot(dmat[...], tok[:, at], preferred_element_type=f32).astype(bf16)
            xs[:, e, :, at] = got.reshape(groups, cap, blk)
            return 0

        lax.fori_loop(0, dim // blk, columns, 0)
        @pl.when(e == 1)
        def _():
            for p in SENDS:
                x_send(1, p).start()

        @pl.when(e == 3)
        def _():
            @pl.when((me == 3) | (me == 1))
            def _():
                hop_send(3).start()
                far_send(2, 0, cap).start()
                if HOP < cap:
                    far_send(3, 0, cap - HOP).start()

            @pl.when((me != 3) & (me != 1))
            def _():
                x_send(2, 2).start()

            for p in SENDS[1:]:
                x_send(2, p).start()

        xr[0, e] = xs[0, e]
        return 0

    lax.fori_loop(1, experts_here, dispatch, 0)

    small[4].wait()
    logits = lax.dot_general(wg[...], tok[...], (((1,), (1,)), ((), ())), preferred_element_type=f32)
    top = jnp.max(logits, axis=0, keepdims=True)
    expd = jnp.exp(logits - top)
    probs = expd / jnp.sum(expd, axis=0, keepdims=True)
    id1, id2, kept2 = ids[0:1, :], ids[1:2, :], keep[0:1, :] > 0
    is1, is2 = expert_row == id1, (expert_row == id2) & kept2

    def pick(mask, value):
        return jnp.sum(jnp.where(mask, value, 0.0), axis=0, keepdims=True)

    gate1, gate2 = pick(is1, probs), pick(is2, probs)
    slot1, slot2 = pick(is1, slot_of[...]), pick(is2, slot_of[...])
    total = gate1 + gate2
    gates[0:1, :] = jnp.where(slot1 < cap, id1.astype(f32) * cap + slot1, -1.0)
    gates[1:2, :] = jnp.where((slot2 < cap) & kept2, id2.astype(f32) * cap + slot2, -1.0)
    gates[2:3, :] = gate1 / total
    gates[3:4, :] = gate2 / total
    gates[4:, :] = jnp.zeros((gates.shape[0] - 4, tokens), f32)
    cols[...] = gates[...].T

    for i, order in enumerate(CW_BLOCKS):
        lane = lax.broadcasted_iota(jnp.int32, (8, 2 * rows), 1)
        slot = lane
        for b, (p, e) in enumerate(order):
            slot = slot + jnp.where(lane // cap == b, first_slot(e, p) - b * cap, 0)
        slots[i] = slot.astype(f32)

    def weights(i, _):
        def block(t, _):
            at = pl.ds(pl.multiple_of(t * blk, blk), blk)
            slot = slots[i, 0:1, :]
            part = cols[at, :]
            cw[i, at, :] = (
                jnp.where(slot == part[:, 0:1], part[:, 2:3], 0.0) + jnp.where(slot == part[:, 1:2], part[:, 3:4], 0.0)
            ).astype(bf16)
            return 0

        return lax.fori_loop(0, tokens // blk, block, 0)

    lax.fori_loop(0, experts_here // 2, weights, 0)

    def expert(e, _):
        s = e % 2
        for i, (start, _count) in enumerate(X_PIECES):
            @pl.when(e == start)
            def _():
                x_wait(i)

        wi_copy(e).wait()

        @pl.when((e == 1) & ((me == 7) | (me == 5)))
        def _():
            hop_send(3).wait_recv()
            hop_on(3).start()

        def up(j, _):
            at = pl.ds(pl.multiple_of(j * blk, blk), blk)
            pre = jnp.dot(xr[:, e].reshape(rows, dim), wi[s, :, at], preferred_element_type=f32)
            hid[:, at] = jnp.maximum(pre, 0.0).astype(bf16)
            return 0

        lax.fori_loop(0, hidden // blk, up, 0)

        @pl.when(e + 2 < experts_here)
        def _():
            wi_copy(e + 2).start()

        wo_copy(e).wait()

        def down(n, _):
            at = pl.ds(pl.multiple_of(n * blk, blk), blk)
            got = jnp.dot(hid[...], wo[s, :, at], preferred_element_type=f32).astype(bf16)
            ys[:, e, :, at] = got.reshape(groups, cap, blk)
            return 0

        lax.fori_loop(0, dim // blk, down, 0)

        @pl.when(e + 2 < experts_here)
        def _():
            wo_copy(e + 2).start()

        @pl.when(e == 1)
        def _():
            for p in SENDS:
                y_send(0, p).start()

        @pl.when(e == 2)
        def _():
            for p in NEAR:
                y_send(1, p).start()

        @pl.when(e == 3)
        def _():
            for p in FAR:
                y_send(2, p).start()

        @pl.when((e == 3) & (me % 2 == 0))
        def _():
            for p in NEAR:
                end_send(p, 0, cap).start()

        @pl.when((e == 3) & (me % 2 == 1))
        def _():
            for p, first, count in [(p, 0, cap - HELD) for p in (4, 5)] + [(p, 0, cap) for p in (6, 7)] + [(p, cap - HELD, HELD) for p in (4, 5)]:
                end_send(p, first, count).start()

        yr[0, e] = ys[0, e]
        return 0

    lax.fori_loop(0, experts_here, expert, 0)

    y_wait(0, 1, groups - 1)

    def columns(n, _):
        at = pl.ds(pl.multiple_of(n * blk, blk), blk)
        acc[:, at] = jnp.dot(cw[0], yr[:, 0:2, :, at].reshape(2 * rows, blk), preferred_element_type=f32)
        return 0

    lax.fori_loop(0, dim // blk, columns, 0)
    def add_rows(first, back_of):
        def part(n, _):
            at = pl.ds(pl.multiple_of(n * blk, blk), blk)
            acc[:, at] += jnp.dot(cw[1, :, first:first + 4 * cap], back_of(at).reshape(4 * cap, blk), preferred_element_type=f32)
            return 0

        lax.fori_loop(0, dim // blk, part, 0)

    y_wait(1, 4, 4)
    add_rows(rows, lambda at: yr[4:8, 2, :, at])
    y_wait(2, 1, 3)
    add_rows(0, lambda at: yr[0:2, 2:4, :, at])
    add_rows(4 * cap, lambda at: yr[2:4, 2:4, :, at])
    cw_end[...] = cw[1, :, 2 * rows - 4 * cap:]
    @pl.when((me == 7) | (me == 5))
    def _():
        hop_on(3).wait_send()

    sent = pl.ds(1, groups - 1)
    copy_to(1, ys.at[4:8, 0], y_end, sent_sem.at[0], yr_sem.at[3]).wait_recv()
    everything = out_rows.at[:, sent]
    copy_to(1, everything, everything, sent_sem.at[0], xr_sem.at[0]).wait_send()


def finish_kernel(acc, cw, y, out, buf, sem):
    blk = buf.shape[0] // 8
    for t in range(8):
        at = pl.ds(t * blk, blk)
        buf[at, :] = (acc[at, :] + jnp.dot(cw[at, :], y[...].reshape(cw.shape[1], acc.shape[1]), preferred_element_type=jnp.float32)).astype(out.dtype)
        pltpu.make_async_copy(buf.at[at], out.at[at], sem.at[0]).start()
    pltpu.make_async_copy(buf, out, sem.at[0]).wait()


def solution(mesh):
    def local_layer(tokens, w_gate, expert_ids, keep_second, w_in, w_out):
        _, token_count, dim = tokens.shape
        experts = w_gate.shape[1]
        here, _, hidden = w_in.shape
        cap = 2 * token_count // experts
        groups = experts // here
        rows = groups * cap
        f32, bf16 = jnp.float32, jnp.bfloat16
        vmem, dma = pltpu.VMEM, pltpu.SemaphoreType.DMA
        acc, cw_end, y_end = pl.pallas_call(
            functools.partial(layer_kernel, cap),
            out_shape=(vmem((token_count, dim), f32), vmem((token_count, 4 * cap), bf16), vmem((4, cap, dim), bf16)),
            in_specs=[pl.BlockSpec(memory_space=pl.ANY)] * 6,
            out_specs=[pl.BlockSpec(memory_space=vmem)] * 3,
            scratch_shapes=[
                vmem((token_count, dim), bf16),
                vmem((experts, dim), bf16),
                vmem((2, token_count), jnp.int32),
                vmem((1, token_count), jnp.int32),
                vmem((experts, token_count), f32),
                vmem((128, token_count), f32),
                vmem((token_count, 128), f32),
                vmem((2, 8, 2 * rows), f32),
                vmem((HOP, dim), bf16),
                vmem((rows, token_count), bf16),
                vmem((2, groups, here, cap, dim), bf16),
                vmem((groups, here, cap, dim), bf16),
                vmem((groups, here, cap, dim), bf16),
                vmem((rows, hidden), bf16),
                vmem((2, dim, hidden), bf16),
                vmem((2, hidden, dim), bf16),
                vmem((here // 2, token_count, 2 * rows), bf16),
                dma((3,)), dma((2,)), dma((2,)),
                dma((1,)), dma((3,)), dma((4,)), dma((2,)),
            ],
            compiler_params=pltpu.CompilerParams(collective_id=0, has_side_effects=True, vmem_limit_bytes=56 * 2**20),
            name="moe_layer",
        )(tokens[0], w_gate.T, expert_ids[0].T, keep_second, w_in, w_out)
        out = pl.pallas_call(
            finish_kernel,
            out_shape=jax.ShapeDtypeStruct((token_count, dim), bf16),
            in_specs=[pl.BlockSpec(memory_space=vmem)] * 3,
            out_specs=pl.BlockSpec(memory_space=pl.ANY),
            scratch_shapes=[vmem((token_count, dim), bf16), dma((1,))],
            compiler_params=pltpu.CompilerParams(vmem_limit_bytes=8 * 2**20),
            name="moe_finish",
        )(acc, cw_end, y_end)
        return out[None]

    group_spec = P(("dp", "ep"))
    return jax.shard_map(local_layer, mesh=mesh, in_specs=(group_spec, P(), group_spec, group_spec, P("ep"), P("ep")), out_specs=group_spec, check_vma=False)
```
